256 devices in a mesh: seq: 32 (over y, x, core), tensor: 8 (over z).
Axes of the slice: x: 4, y: 4, z: 8, core: 2. Of those that a mesh axis runs over, the one named last changes fastest.
Arguments:
- streams: float32 [4, 16384, 4096], P(None, 'seq', 'tensor'), may hold values from -8 to 8
- mix_weight: float32 [24, 4, 4096], P(None, None, 'tensor'), may hold values from -0.046875 to 0.046875
- mix_bias: float32 [24], replicated, may hold values from -4 to 4
- mix_scale: float32 [3], replicated, may hold values from 1 to 2
- norm_gain: bfloat16 [4096], replicated, may hold values from 0.25 to 1.75
- gate_weight: bfloat16 [4096, 7168], P('seq', 'tensor'), may hold values from -0.09375 to 0.09375
- up_weight: bfloat16 [4096, 7168], P('seq', 'tensor'), may hold values from -0.09375 to 0.09375
- down_weight: bfloat16 [7168, 4096], P('tensor', 'seq'), may hold values from -0.0625 to 0.0625
Outputs:
- new_streams: float32 [4, 16384, 4096], P(None, 'seq', 'tensor')
The draws below stay inside these ranges and needn't reach their ends.
All inputs are finite; a program needn't handle non-finite values.
Results may differ from the reference program's by a relative error of at most 0.01.
Values may be sent and summed in bfloat16 or wider, within the bound.
A program may use at most 128 MiB of HBM per device.

```python
import jax
import jax.numpy as jnp
from jax import lax

D = 4096
FF = 7168
STREAMS = 4
SWEEPS = 20
TOK_DEV = 512
TOKENS = 16384
LOGITS = 24
N_SEQ = 32
N_TENSOR = 8


def draw_streams(key, part):
    first = jax.random.fold_in(key, 11)
    second = jax.random.fold_in(key, 12)
    fifth = jax.random.fold_in(key, 15)
    groups = max(D // 64, 1)
    columns = D // groups
    scales = jnp.exp(jax.random.uniform(second, (STREAMS, TOKENS, groups, 1), jnp.float32, -1.2, 1.2))
    coarse = jnp.exp(jax.random.uniform(fifth, (STREAMS, TOKENS, 8, 1), jnp.float32, -1.5, 1.5))
    values = jax.random.normal(first, (STREAMS, TOKENS, groups, columns), jnp.float32) * scales
    values = values.reshape(STREAMS, TOKENS, 8, D // 8) * coarse
    return jnp.clip(values, -8.0, 8.0).reshape(STREAMS, TOKENS, D)


def steps_of(stream_key, dims, shards, least, high):
    level, own = 1.0, jax.random.fold_in(stream_key, 6)
    for dim, blocks in shards:
        steps = jnp.exp(jax.random.uniform(jax.random.fold_in(own, dim), (blocks,), jnp.float32, least / len(shards), high / len(shards)))
        level = level * jnp.repeat(steps, dims[dim] // blocks).reshape([-1 if axis == dim else 1 for axis in range(len(dims))])
    return level


def noise(own_key, shape, scale, bound, cuts=(), kind=jnp.bfloat16):
    array = scale * jax.random.normal(own_key, shape, jnp.float32)
    if cuts:
        array = array * steps_of(own_key, shape, cuts, -0.22, 0.18)
    return jnp.clip(array, -bound, bound).astype(kind)


def setup_inputs(seed: int = 0) -> dict:
    keys = jax.random.split(jax.random.key(seed), 9)
    return {
        "streams": draw_streams(jax.random.fold_in(keys[8], 71), 0),
        "mix_weight": noise(keys[1], (LOGITS, STREAMS, D), (STREAMS * D) ** -0.5, 0.046875, ((2, 8),), jnp.float32),
        "mix_bias": noise(keys[2], (LOGITS,), 1.0, 4.0, (), jnp.float32),
        "mix_scale": jnp.clip(jax.random.uniform(keys[3], (3,), jnp.float32, 1.0, 2.0), 1.0, 2.0),
        "norm_gain": jnp.clip(1.0 + 0.15 * jax.random.normal(keys[4], (D,), jnp.float32), 0.25, 1.75).astype(jnp.bfloat16),
        "gate_weight": noise(keys[5], (D, FF), D ** -0.5, 0.09375, ((0, 32), (1, 8))),
        "up_weight": noise(keys[6], (D, FF), D ** -0.5, 0.09375, ((0, 32), (1, 8))),
        "down_weight": noise(keys[7], (FF, D), FF ** -0.5, 0.0625, ((0, 8), (1, 32))),
    }


epsilon = 0.25

def coefficients(logits, mix_bias, mix_scale):
    pre_mix = jax.nn.sigmoid(mix_scale[0] * logits[:STREAMS] + mix_bias[:STREAMS, None])
    post_mix = 2.0 * jax.nn.sigmoid(mix_scale[1] * logits[STREAMS:2 * STREAMS] + mix_bias[STREAMS:2 * STREAMS, None])
    start_mix = jnp.exp(mix_scale[2] * logits[2 * STREAMS:] + mix_bias[2 * STREAMS:, None])
    start_mix = start_mix.reshape(STREAMS, STREAMS, logits.shape[1])

    def balance(iteration, matrix):
        matrix = matrix / lax.optimization_barrier(jnp.sum(matrix, axis=1, keepdims=True))
        return matrix / lax.optimization_barrier(jnp.sum(matrix, axis=0, keepdims=True))
    return (pre_mix, post_mix, lax.fori_loop(0, SWEEPS, balance, start_mix))

def layer_block(block, streams, mix_weight, mix_bias, mix_scale, norm_gain, gate_weight, up_weight, down_weight):
    current = lax.dynamic_slice_in_dim(streams, (block * TOK_DEV).astype(jnp.int32), TOK_DEV, 1)
    squares = lax.optimization_barrier(jnp.sum(current * current, axis=(0, 2)))
    inverse = lax.rsqrt(squares / (STREAMS * D) + epsilon)
    raw_logits = jnp.einsum('lkd,ktd->lt', mix_weight, current, precision=lax.Precision.HIGHEST)
    pre_mix, post_mix, res_mix = coefficients(raw_logits * inverse[None, :], mix_bias, mix_scale)
    layer_in = lax.optimization_barrier(jnp.sum(pre_mix[:, :, None] * current, axis=0)).astype(jnp.bfloat16)
    as_float = layer_in.astype(jnp.float32)
    mean_square = lax.optimization_barrier(jnp.mean(as_float * as_float, axis=1, keepdims=True))
    normed = (as_float * lax.rsqrt(mean_square + epsilon) * norm_gain.astype(jnp.float32)).astype(jnp.bfloat16)
    gate_value = jnp.dot(normed, gate_weight, preferred_element_type=jnp.float32)
    up_value = jnp.dot(normed, up_weight, preferred_element_type=jnp.float32)
    hidden = (jax.nn.silu(gate_value) * up_value).astype(jnp.bfloat16)
    share = FF // N_TENSOR
    layer_out = jnp.zeros((TOK_DEV, D), jnp.float32)
    for group in range(N_TENSOR):
        partial_out = jnp.dot(hidden[:, group * share:(group + 1) * share], down_weight[group * share:(group + 1) * share], preferred_element_type=jnp.float32)
        rounded = lax.optimization_barrier(partial_out.astype(jnp.bfloat16))
        layer_out = layer_out + rounded.astype(jnp.float32)
    outputs = []
    for target in range(STREAMS):
        mixed = post_mix[target][:, None] * layer_out
        for source in range(STREAMS):
            mixed = mixed + res_mix[target, source][:, None] * current[source]
        outputs.append(mixed)
    return jnp.stack(outputs)

def reference(streams, mix_weight, mix_bias, mix_scale, norm_gain, gate_weight, up_weight, down_weight):

    def one_block(block):
        return layer_block(block, streams, mix_weight, mix_bias, mix_scale, norm_gain, gate_weight, up_weight, down_weight)
    blocks = lax.map(one_block, jnp.arange(N_SEQ, dtype=jnp.int32))
    return jnp.moveaxis(blocks, 0, 1).reshape(STREAMS, TOKENS, D)
```

```python
import functools

import jax
import jax.numpy as jnp
from jax import lax
from jax.experimental import pallas as pl
from jax.experimental.pallas import tpu as pltpu
from jax.sharding import PartitionSpec as P

STREAMS = 4
SWEEPS = 20
EPSILON = 0.25
MESH = pl.DeviceIdType.MESH
NX = 4
NY = 4
NZ = 8
TOK = 512
COLS = 512
ROWS = 128
FFL = 896
CHUNKS = 4
CT = TOK // CHUNKS
PERM = (0, 2, 1, 3)
F32 = jnp.float32
BF16 = jnp.bfloat16


def wrap(value, size):
    return lax.rem(value + size, size)


def nt_dot(a, b, precision=None):
    return lax.dot_general(
        a, b, (((1,), (1,)), ((), ())), precision=precision, preferred_element_type=F32
    )


def kernel(
    st_hbm, mw, bias, scale, gain, g_hbm, u_hbm, d_hbm, out_hbm,
    st, wg, wu, wd, xg, hid, rr, rl, sr, sl, pst, ost, sqx, pre_t, coef_t, inv_t, outb, tmp,
    loc_sem, out_sem, w_send, w_recv, ag_send, ag_recv, rs_send, rs_recv,
    ps_send, ps_recv, os_send, os_recv, sq_send, sq_recv,
):
    s = lax.axis_index("seq")
    z = lax.axis_index("tensor")
    core = lax.rem(s, 2)
    x = lax.rem(lax.div(s, 2), NX)
    y = lax.div(s, 2 * NX)

    def at(xx, yy, cc):
        return {"seq": (yy * NX + xx) * 2 + cc, "tensor": z}

    xp, xm = wrap(x + 1, NX), wrap(x - 1, NX)
    yp, ym = wrap(y + 1, NY), wrap(y - 1, NY)
    x_up, x_dn = at(xp, y, core), at(xm, y, core)
    y_up, y_dn = at(x, yp, core), at(x, ym, core)
    other = at(x, y, 1 - core)
    right = {"seq": s, "tensor": wrap(z + 1, NZ)}
    left = {"seq": s, "tensor": wrap(z - 1, NZ)}
    z_peers = {d: {"seq": s, "tensor": wrap(z + d, NZ)} for d in range(1, NZ)}

    st_copies = [
        pltpu.make_async_copy(
            st_hbm.at[:, pl.ds(c * CT, CT), :], st.at[:, pl.ds(c * CT, CT), :], loc_sem.at[c]
        )
        for c in range(CHUNKS)
    ]
    w_copies = [
        pltpu.make_async_copy(src, dst.at[core, y, x], loc_sem.at[CHUNKS + i])
        for i, (src, dst) in enumerate(((g_hbm, wg), (u_hbm, wu), (d_hbm, wd)))
    ]
    for c in w_copies:
        c.start()
    for c in st_copies:
        c.start()

    barrier = pltpu.get_barrier_semaphore()
    peers = [x_up, x_dn, y_up, y_dn, other] + [z_peers[d] for d in range(1, NZ)]
    for peer in peers:
        pl.semaphore_signal(barrier, inc=1, device_id=peer, device_id_type=MESH)
    pl.semaphore_wait(barrier, len(peers))

    sends = []

    def remote(ref, send_sem, recv_sem, dev):
        return pltpu.make_async_remote_copy(
            src_ref=ref, dst_ref=ref, send_sem=send_sem, recv_sem=recv_sem,
            device_id=dev, device_id_type=MESH,
        )

    items = (
        (wg, 0, ROWS, True),
        (wu, 0, ROWS, False),
        (wd, 0, FFL // 2, True),
        (wd, FFL // 2, FFL // 2, False),
    )

    def w_region(i, cc, f, sec, start, count, r0, nr):
        ref, base, rows, x_first = items[i]
        rsl = pl.ds(base + r0, nr)
        if x_first:
            return ref.at[cc, sec, pl.ds(f, count) if count > 1 else f, rsl, :]
        return ref.at[cc, pl.ds(f, count) if count > 1 else f, sec, rsl, :]

    def axes(i):
        if items[i][3]:
            return x, y, x_up, x_dn, y_up, y_dn
        return y, x, y_up, y_dn, x_up, x_dn

    def w_copy(i, k, dev, region):
        return remote(region, w_send.at[i, k], w_recv.at[i, k], dev)

    def w_go(i, k, dev, region):
        c = w_copy(i, k, dev, region)
        c.start()
        sends.append(c)

    def w_got(i, k, region):
        w_copy(i, k, other, region).wait_recv()

    def step1(i):
        f, sec, f_up, f_dn, _, _ = axes(i)
        rows = items[i][2]
        own = w_region(i, core, f, sec, 0, 1, 0, rows)
        w_go(i, 0, f_up, own)
        w_go(i, 1, f_dn, own)

    def step2(i):
        f, sec, f_up, f_dn, _, _ = axes(i)
        rows = items[i][2]
        half = rows // 2
        fm, fp = wrap(f - 1, 4), wrap(f + 1, 4)
        w_got(i, 0, w_region(i, core, fm, sec, 0, 1, 0, rows))
        w_go(i, 2, f_up, w_region(i, core, fm, sec, 0, 1, 0, half))
        w_got(i, 1, w_region(i, core, fp, sec, 0, 1, 0, rows))
        w_go(i, 3, f_dn, w_region(i, core, fp, sec, 0, 1, half, half))

    def row_to_other(i, k, sec):
        w_go(i, k, other, w_region(i, core, 0, sec, 0, 4, 0, items[i][2]))

    def step2_end(i):
        f, sec, _, _, _, _ = axes(i)
        half = items[i][2] // 2
        f2 = wrap(f + 2, 4)
        w_got(i, 2, w_region(i, core, f2, sec, 0, 1, 0, half))
        w_got(i, 3, w_region(i, core, f2, sec, 0, 1, half, half))

    def pair(i, cc, p, sec):
        return w_region(i, cc, 2 * p, sec, 0, 2, 0, items[i][2])

    def step3(i):
        _, sec, _, _, s_up, s_dn = axes(i)
        w_go(i, 4, s_up, pair(i, core, 0, sec))
        w_go(i, 7, s_dn, pair(i, core, 1, sec))
        w_go(i, 5, s_up, pair(i, core, 1, sec))
        w_go(i, 6, s_dn, pair(i, core, 0, sec))

    def step4(i):
        _, sec, _, _, s_up, s_dn = axes(i)
        sm, sp = wrap(sec - 1, 4), wrap(sec + 1, 4)
        w_got(i, 4, pair(i, core, 0, sm))
        w_go(i, 8, s_up, pair(i, core, 0, sm))
        w_got(i, 7, pair(i, core, 1, sp))
        w_go(i, 9, s_dn, pair(i, core, 1, sp))

    def step4_mid(i):
        _, sec, _, _, _, _ = axes(i)
        sm, sp = wrap(sec - 1, 4), wrap(sec + 1, 4)
        w_got(i, 5, pair(i, core, 1, sm))
        row_to_other(i, 11, sm)
        w_got(i, 6, pair(i, core, 0, sp))
        row_to_other(i, 12, sp)

    def step4_end(i):
        _, sec, _, _, _, _ = axes(i)
        s2 = wrap(sec + 2, 4)
        w_got(i, 8, pair(i, core, 0, s2))
        w_got(i, 9, pair(i, core, 1, s2))
        row_to_other(i, 13, s2)

    def others_rows(i):
        _, sec, _, _, _, _ = axes(i)
        for k, sec_k in ((10, sec), (11, wrap(sec - 1, 4)), (12, wrap(sec + 1, 4)), (13, wrap(sec + 2, 4))):
            w_got(i, k, w_region(i, 1 - core, 0, sec_k, 0, 4, 0, items[i][2]))

    def own_row_to_other(i):
        row_to_other(i, 10, axes(i)[1])

    for c in w_copies:
        c.wait()
    for i in range(4):
        step1(i)

    ones = jnp.ones((8, 128), F32)
    for c in range(CHUNKS):
        st_copies[c].wait()
        tok = pl.ds(c * CT, CT)
        squares = jnp.zeros((CT, COLS), F32)
        raw = jnp.zeros((24, CT), F32)
        for k in range(STREAMS):
            v = st[k, tok, :]
            squares = squares + v * v
            raw = raw + nt_dot(mw[:, k, :], v)
        squares = (squares[:, :128] + squares[:, 128:256]) + (squares[:, 256:384] + squares[:, 384:])
        sq_row = nt_dot(ones, squares, lax.Precision.HIGHEST)
        pst[z, 0:4, tok] = raw[0:4]
        pst[z, 4:8, tok] = sq_row[4:8]
        ost[z, 0:20, tok] = raw[4:24]
        ost[z, 20:24, tok] = sq_row[4:8]
    for d in (4, 3, 5, 2, 6, 1, 7):
        c = remote(pst.at[z], ps_send.at[d], ps_recv.at[d], z_peers[d])
        c.start()
        sends.append(c)
    for d in (4, 3, 5, 2, 6, 1, 7):
        c = remote(ost.at[z], os_send.at[d], os_recv.at[d], z_peers[d])
        c.start()
        sends.append(c)
    for d in range(1, NZ):
        remote(pst.at[wrap(z - d, NZ)], ps_send.at[d], ps_recv.at[d], z_peers[d]).wait_recv()

    total = pst[0]
    for o in range(1, NZ):
        total = total + pst[o]
    inverse = lax.rsqrt(total[4:5] / float(STREAMS * COLS * NZ) + EPSILON)
    row8 = lax.broadcasted_iota(jnp.int32, (8, 1), 0)
    bias8 = jnp.zeros((8, 1), F32)
    for l in range(4):
        bias8 = jnp.where(row8 == l, bias[l], bias8)
    pre = jax.nn.sigmoid(scale[0] * (total * inverse) + bias8)
    pre = jnp.concatenate([pre, jnp.zeros((120, TOK), F32)], axis=0)
    pre_t[...] = pre.T

    def hops(c, to_right):
        return 4 if (c % 2 == 0) == to_right else 3

    def ag_copy(c, h, to_right, origin):
        q = 0 if to_right else 1
        return remote(
            xg.at[origin, pl.ds(c * CT, CT), :], ag_send.at[q, c, h], ag_recv.at[q, c, h],
            right if to_right else left,
        )

    def ag_go(c, h, to_right, origin):
        cp = ag_copy(c, h, to_right, origin)
        cp.start()
        sends.append(cp)

    g_row = gain[z]
    for c in range(CHUNKS):
        tok = pl.ds(c * CT, CT)
        layer_in = pre_t[tok, 0:1] * st[0, tok, :]
        for k in range(1, STREAMS):
            layer_in = layer_in + pre_t[tok, k : k + 1] * st[k, tok, :]
        sent = (layer_in * g_row).astype(BF16)
        for q in range(4):
            xg[z, tok, q * 128 : (q + 1) * 128] = sent[:, PERM[q] * 128 : (PERM[q] + 1) * 128]
        ag_go(c, 0, True, z)
        ag_go(c, 0, False, z)
        sq = layer_in * layer_in
        sq = (sq[:, :128] + sq[:, 128:256]) + (sq[:, 256:384] + sq[:, 384:])
        sqx[z, :, tok] = nt_dot(ones, sq, lax.Precision.HIGHEST)[0:1]
    for d in (4, 3, 5, 2, 6, 1, 7):
        c = remote(sqx.at[z], sq_send.at[d], sq_recv.at[d], z_peers[d])
        c.start()
        sends.append(c)

    def ag_step(h):
        for c in range(CHUNKS):
            for to_right in (True, False):
                if h < hops(c, to_right):
                    origin = wrap(z - (h + 1), NZ) if to_right else wrap(z + (h + 1), NZ)
                    ag_copy(c, h, to_right, origin).wait_recv()
                    if h + 1 < hops(c, to_right):
                        ag_go(c, h + 1, to_right, origin)

    for i in range(4):
        step2(i)
    for i in range(2):
        step2_end(i)
        step3(i)
        own_row_to_other(i)
    for i in range(2, 4):
        step2_end(i)
        own_row_to_other(i)

    for d in range(1, NZ):
        remote(ost.at[wrap(z - d, NZ)], os_send.at[d], os_recv.at[d], z_peers[d]).wait_recv()
    rest = ost[0]
    for o in range(1, NZ):
        rest = rest + ost[o]
    rest = rest * inverse
    row4 = lax.broadcasted_iota(jnp.int32, (4, 1), 0)

    def bias4(first):
        b = jnp.full((4, 1), bias[first], F32)
        for l in range(1, 4):
            b = jnp.where(row4 == l, bias[first + l], b)
        return b

    post = 2.0 * jax.nn.sigmoid(scale[1] * rest[0:4] + bias4(4))
    mix = tuple(
        jnp.exp(scale[2] * rest[4 + 4 * k : 8 + 4 * k] + bias4(8 + 4 * k)) for k in range(4)
    )

    def balance(_, m):
        m = tuple(v / jnp.sum(v, axis=0, keepdims=True) for v in m)
        col = (m[0] + m[1]) + (m[2] + m[3])
        return tuple(v / col for v in m)

    mix = lax.fori_loop(0, SWEEPS, balance, mix)
    coef = jnp.concatenate((post,) + mix + (jnp.zeros((108, TOK), F32),), axis=0)
    coef_t[...] = coef.T

    ag_step(0)
    for i in range(2):
        step4(i)
    for i in range(2, 4):
        step3(i)
    ag_step(1)
    for i in range(2):
        step4_mid(i)
    for d in range(1, NZ):
        remote(sqx.at[wrap(z - d, NZ)], sq_send.at[d], sq_recv.at[d], z_peers[d]).wait_recv()
    sq_total = sqx[0]
    for o in range(1, NZ):
        sq_total = sq_total + sqx[o]
    inv = lax.rsqrt(sq_total / float(COLS * NZ) + EPSILON)
    inv_t[...] = jnp.broadcast_to(inv, (128, TOK)).T
    ag_step(2)
    for i in range(2):
        step4_end(i)
    for i in range(2, 4):
        step4(i)
    for i in range(2):
        others_rows(i)
    ag_step(3)

    halves = 2
    ht = TOK // halves
    n_tiles = FFL // 128

    def gate_up(half):
        def tile(n, carry):
            tok = pl.ds(half * ht, ht)
            lanes = pl.ds(pl.multiple_of(n * 128, 128), 128)
            acc = None
            for b in range(NZ):
                for cc in range(2):
                    a = xg[b, tok, cc * 256 : (cc + 1) * 256]
                    j = 2 * (b % 2)
                    bg = wg[cc, b // 2, j : j + 2, :, lanes].reshape(256, 128)
                    bu = wu[cc, b // 2, j : j + 2, :, lanes].reshape(256, 128)
                    d = jnp.dot(a, jnp.concatenate([bg, bu], axis=1), preferred_element_type=F32)
                    acc = d if acc is None else acc + d
            scale_t = inv_t[tok, :]
            g = acc[:, :128] * scale_t
            u = acc[:, 128:] * scale_t
            hid[tok, lanes] = (g / (1.0 + jnp.exp(-g)) * u).astype(BF16)
            return carry

        lax.fori_loop(0, n_tiles, tile, 0)

    gate_up(0)
    for i in range(2, 4):
        step4_mid(i)
    gate_up(1)
    for i in range(2, 4):
        step4_end(i)
    for i in range(2, 4):
        others_rows(i)

    def partial(dest, tok):
        a = hid[tok, :]
        parts = []
        j = 2 * lax.rem(dest, 2)
        for cc in range(2):
            b0 = wd[cc, lax.div(dest, 2), j]
            b1 = wd[cc, lax.div(dest, 2), j + 1]
            parts.append(
                jnp.dot(a, jnp.concatenate([b0, b1], axis=1), preferred_element_type=F32)
            )
        return parts

    def rs_copy(q, c, t):
        src, dst = (sr, rr) if q == 0 else (sl, rl)
        return pltpu.make_async_remote_copy(
            src_ref=src.at[c, t], dst_ref=dst.at[c, t],
            send_sem=rs_send.at[q, c, t], recv_sem=rs_recv.at[q, c, t],
            device_id=right if q == 0 else left, device_id_type=MESH,
        )

    def rs_body(idx, carry):
        t = lax.div(idx, CHUNKS)
        c = lax.rem(idx, CHUNKS)
        odd = lax.rem(c, 2)
        tok = pl.ds(pl.multiple_of(c * CT, CT), CT)
        for q in range(2):
            n_hops = 4 - odd if q == 0 else 3 + odd

            @pl.when(t < n_hops)
            def _():
                dest = wrap(z + n_hops - t, NZ) if q == 0 else wrap(z - n_hops + t, NZ)
                p0, p1 = partial(dest, tok)
                src, dst = (sr, rr) if q == 0 else (sl, rl)

                @pl.when(t == 0)
                def _():
                    src[c, t, :, 0:256] = p0.astype(BF16)
                    src[c, t, :, 256:512] = p1.astype(BF16)

                @pl.when(t > 0)
                def _():
                    tmp[:, 0:256] = p0
                    tmp[:, 256:512] = p1
                    rs_copy(q, c, t - 1).wait_recv()
                    src[c, t] = (tmp[...] + dst[c, t - 1].astype(F32)).astype(BF16)

                rs_copy(q, c, t).start()

        return carry

    lax.fori_loop(0, 4 * CHUNKS, rs_body, 0)

    def out_copy(c):
        tok = pl.ds(pl.multiple_of(c * CT, CT), CT)
        return pltpu.make_async_copy(outb.at[:, tok, :], out_hbm.at[:, tok, :], out_sem.at[c])

    def out_body(c, carry):
        odd = lax.rem(c, 2)
        tok = pl.ds(pl.multiple_of(c * CT, CT), CT)
        p0, p1 = partial(z, tok)
        tmp[:, 0:256] = p0
        tmp[:, 256:512] = p1
        rs_copy(0, c, 3 - odd).wait_recv()
        rs_copy(1, c, 2 + odd).wait_recv()
        tmp[...] = (
            tmp[...] + rr[c, 3 - odd].astype(F32) + rl[c, 2 + odd].astype(F32)
        )
        for k in range(STREAMS):
            for q in range(4):
                lanes = slice(PERM[q] * 128, (PERM[q] + 1) * 128)
                v = coef_t[tok, k : k + 1] * tmp[:, q * 128 : (q + 1) * 128]
                for j in range(STREAMS):
                    col = 4 + 4 * k + j
                    v = v + coef_t[tok, col : col + 1] * st[j, tok, lanes]
                outb[k, tok, lanes] = v
        out_copy(c).start()
        return carry

    lax.fori_loop(0, CHUNKS, out_body, 0)

    for c in sends:
        c.wait_send()

    def drain(idx, carry):
        t = lax.div(idx, CHUNKS)
        c = lax.rem(idx, CHUNKS)
        odd = lax.rem(c, 2)
        for q in range(2):
            n_hops = 4 - odd if q == 0 else 3 + odd

            @pl.when(t < n_hops)
            def _():
                rs_copy(q, c, t).wait_send()

        return carry

    lax.fori_loop(0, 4 * CHUNKS, drain, 0)
    for c in range(CHUNKS):
        out_copy(c).wait()


def body(streams, mix_weight, mix_bias, mix_scale, norm_gain, gate_weight, up_weight, down_weight):
    gain = norm_gain.astype(F32).reshape(NZ, 1, COLS)
    any_space = pl.BlockSpec(memory_space=pl.ANY)
    vmem = pl.BlockSpec(memory_space=pltpu.VMEM)
    smem = pl.BlockSpec(memory_space=pltpu.SMEM)
    dma = pltpu.SemaphoreType.DMA
    call = pl.pallas_call(
        kernel,
        out_shape=jax.ShapeDtypeStruct((STREAMS, TOK, COLS), F32),
        in_specs=[any_space, vmem, smem, smem, vmem, any_space, any_space, any_space],
        out_specs=any_space,
        scratch_shapes=[
            pltpu.VMEM((STREAMS, TOK, COLS), F32),
            pltpu.VMEM((2, NY, NX, ROWS, FFL), BF16),
            pltpu.VMEM((2, NY, NX, ROWS, FFL), BF16),
            pltpu.VMEM((2, NY, NX, FFL, 128), BF16),
            pltpu.VMEM((NZ, TOK, COLS), BF16),
            pltpu.VMEM((TOK, FFL), BF16),
            pltpu.VMEM((CHUNKS, 4, CT, COLS), BF16),
            pltpu.VMEM((CHUNKS, 4, CT, COLS), BF16),
            pltpu.VMEM((CHUNKS, 4, CT, COLS), BF16),
            pltpu.VMEM((CHUNKS, 4, CT, COLS), BF16),
            pltpu.VMEM((NZ, 8, TOK), F32),
            pltpu.VMEM((NZ, 24, TOK), F32),
            pltpu.VMEM((NZ, 1, TOK), F32),
            pltpu.VMEM((TOK, 128), F32),
            pltpu.VMEM((TOK, 128), F32),
            pltpu.VMEM((TOK, 128), F32),
            pltpu.VMEM((STREAMS, TOK, COLS), F32),
            pltpu.VMEM((CT, COLS), F32),
            dma((CHUNKS + 3,)),
            dma((CHUNKS,)),
            dma((4, 14)),
            dma((4, 14)),
            dma((2, CHUNKS, 4)),
            dma((2, CHUNKS, 4)),
            dma((2, CHUNKS, 4)),
            dma((2, CHUNKS, 4)),
            dma((8,)),
            dma((8,)),
            dma((8,)),
            dma((8,)),
            dma((8,)),
            dma((8,)),
        ],
        compiler_params=pltpu.CompilerParams(
            collective_id=0, has_side_effects=True, vmem_limit_bytes=62 * 1024 * 1024
        ),
    )
    return call(
        streams, mix_weight, mix_bias, mix_scale, gain, gate_weight, up_weight, down_weight
    )


def solution(mesh):
    placed = (
        P(None, "seq", "tensor"),
        P(None, None, "tensor"),
        P(),
        P(),
        P(),
        P("seq", "tensor"),
        P("seq", "tensor"),
        P("tensor", "seq"),
    )
    return jax.shard_map(
        body, mesh=mesh, in_specs=placed, out_specs=P(None, "seq", "tensor"), check_vma=False
    )
```

```python
import functools

import jax
import jax.numpy as jnp
from jax import lax
from jax.experimental import pallas as pl
from jax.experimental.pallas import tpu as pltpu
from jax.sharding import PartitionSpec as P

STREAMS = 4
SWEEPS = 20
EPSILON = 0.25
MESH = pl.DeviceIdType.MESH
NX = 4
NY = 4
NZ = 8
TOK = 512
COLS = 512
ROWS = 128
FFL = 896
CHUNKS = 4
CT = TOK // CHUNKS
PERM = (0, 2, 1, 3)
F32 = jnp.float32
BF16 = jnp.bfloat16


def wrap(value, size):
    return lax.rem(value + size, size)


def nt_dot(a, b, precision=None):
    return lax.dot_general(
        a, b, (((1,), (1,)), ((), ())), precision=precision, preferred_element_type=F32
    )


def kernel(
    st_hbm, mw, bias, scale, gain, g_hbm, u_hbm, d_hbm, lo, coef_t,
    st, wg, wu, wd, xg, hid, rr, rl, sr, sl, pst, ost, sqx, pre_t, inv_t, tmp, g32,
    loc_sem, w_send, w_recv, ag_send, ag_recv, rs_send, rs_recv,
    ps_send, ps_recv, os_send, os_recv, sq_send, sq_recv,
):
    s = lax.axis_index("seq")
    z = lax.axis_index("tensor")
    core = lax.rem(s, 2)
    x = lax.rem(lax.div(s, 2), NX)
    y = lax.div(s, 2 * NX)

    def at(xx, yy, cc):
        return {"seq": (yy * NX + xx) * 2 + cc, "tensor": z}

    x_up, x_dn = at(wrap(x + 1, NX), y, core), at(wrap(x - 1, NX), y, core)
    y_up, y_dn = at(x, wrap(y + 1, NY), core), at(x, wrap(y - 1, NY), core)
    other = at(x, y, 1 - core)
    right = {"seq": s, "tensor": wrap(z + 1, NZ)}
    left = {"seq": s, "tensor": wrap(z - 1, NZ)}
    z_peers = {d: {"seq": s, "tensor": wrap(z + d, NZ)} for d in range(1, NZ)}
    far_first = (4, 3, 5, 2, 6, 1, 7)

    w_copies = [
        pltpu.make_async_copy(src, dst.at[core, y, x], loc_sem.at[CHUNKS + i])
        for i, (src, dst) in enumerate(((g_hbm, wg), (u_hbm, wu), (d_hbm, wd)))
    ]
    st_copies = [
        pltpu.make_async_copy(
            st_hbm.at[:, pl.ds(c * CT, CT), :], st.at[:, pl.ds(c * CT, CT), :], loc_sem.at[c]
        )
        for c in range(CHUNKS)
    ]
    for c in w_copies[:2] + st_copies + w_copies[2:]:
        c.start()

    barrier = pltpu.get_barrier_semaphore()
    peers = [x_up, x_dn, y_up, y_dn, other] + [z_peers[d] for d in range(1, NZ)]
    for peer in peers:
        pl.semaphore_signal(barrier, inc=1, device_id=peer, device_id_type=MESH)
    g32[...] = gain[...].astype(F32)
    pl.semaphore_wait(barrier, len(peers))

    sends = []

    def remote(ref, send_sem, recv_sem, dev):
        return pltpu.make_async_remote_copy(
            src_ref=ref, dst_ref=ref, send_sem=send_sem, recv_sem=recv_sem,
            device_id=dev, device_id_type=MESH,
        )

    GATE, UP, DOWN = 0, 1, 2
    items = ((wg, ROWS, True), (wu, ROWS, False), (wd, FFL, False))

    def axes(i):
        if items[i][2]:
            return x, y, x_up, x_dn, y_up, y_dn
        return y, x, y_up, y_dn, x_up, x_dn

    def shard(i, f, sec, half=None, cc=None):
        ref, rows, x_first = items[i]
        cc = core if cc is None else cc
        rsl = slice(None) if half is None else pl.ds(half * (rows // 2), rows // 2)
        return ref.at[cc, sec, f, rsl, :] if x_first else ref.at[cc, f, sec, rsl, :]

    def w_copy(i, k, dev, region):
        return remote(region, w_send.at[i, k], w_recv.at[i, k], dev)

    def w_go(i, k, dev, region):
        c = w_copy(i, k, dev, region)
        c.start()
        sends.append(c)

    def w_got(i, k, region):
        w_copy(i, k, other, region).wait_recv()

    zq = lax.div(z, 2)
    zo = lax.rem(z, 2)
    need = [wrap(zq + 2, 4), wrap(zq + 1 + 2 * zo, 4), wrap(zq + 3 - 2 * zo, 4), wrap(zq, 4)]

    def order(i):
        f = axes(i)[0]
        if i == DOWN:
            return need
        return [f, wrap(f - 1, 4), wrap(f + 1, 4), wrap(f + 2, 4)]

    def forwards(i):
        if i == DOWN:
            return ((0, None), (2, 0), (3, 0)), ((1, None), (2, 1), (3, 1))
        return ((0, None), (1, None)), ((2, None), (3, None))

    def step1(i):
        f, sec, f_up, f_dn, _, _ = axes(i)
        w_go(i, 0, f_up, shard(i, f, sec))
        w_go(i, 1, f_dn, shard(i, f, sec))

    def step2(i):
        f, sec, f_up, f_dn, _, _ = axes(i)
        fm, fp = wrap(f - 1, 4), wrap(f + 1, 4)
        w_got(i, 0, shard(i, fm, sec))
        w_go(i, 2, f_up, shard(i, fm, sec, 0))
        w_got(i, 1, shard(i, fp, sec))
        w_go(i, 3, f_dn, shard(i, fp, sec, 1))

    def step2_end(i):
        f, sec = axes(i)[:2]
        w_got(i, 2, shard(i, wrap(f + 2, 4), sec, 0))
        w_got(i, 3, shard(i, wrap(f + 2, 4), sec, 1))

    def half_up(r, n):
        k = 4 + r if n == 0 else 30 + r
        w_go(DOWN, k, axes(DOWN)[4], shard(DOWN, need[r], x, n))

    def half_dn(r, n):
        k = 8 + r if n == 1 else 32 + r
        w_go(DOWN, k, axes(DOWN)[5], shard(DOWN, need[r], x, n))

    def got_half_up(r, n):
        w_got(DOWN, 4 + r if n == 0 else 30 + r, shard(DOWN, need[r], wrap(x - 1, 4), n))

    def got_half_dn(r, n):
        w_got(DOWN, 8 + r if n == 1 else 32 + r, shard(DOWN, need[r], wrap(x + 1, 4), n))

    def fwd_half_up(r):
        got_half_up(r, 0)
        w_go(DOWN, 11 + r, axes(DOWN)[4], shard(DOWN, need[r], wrap(x - 1, 4), 0))

    def fwd_half_dn(r):
        got_half_dn(r, 1)
        w_go(DOWN, 14 + r, axes(DOWN)[5], shard(DOWN, need[r], wrap(x + 1, 4), 1))

    def send_halves(r):
        half_up(r, 0)
        half_dn(r, 1)
        half_up(r, 1)
        half_dn(r, 0)

    def across_up(i, r):
        w_go(i, 4 + r, axes(i)[4], shard(i, order(i)[r], axes(i)[1]))

    def across_dn(i, r):
        w_go(i, 8 + r, axes(i)[5], shard(i, order(i)[r], axes(i)[1]))

    def got_up(i, r):
        w_got(i, 4 + r, shard(i, order(i)[r], wrap(axes(i)[1] - 1, 4)))

    def got_dn(i, r):
        w_got(i, 8 + r, shard(i, order(i)[r], wrap(axes(i)[1] + 1, 4)))

    def fwd_up(i, n):
        r, half = forwards(i)[0][n]
        if n == 0 or forwards(i)[0][n - 1][0] != r:
            got_up(i, r)
        w_go(i, 12 + n, axes(i)[4], shard(i, order(i)[r], wrap(axes(i)[1] - 1, 4), half))

    def fwd_dn(i, n):
        r, half = forwards(i)[1][n]
        got_dn(i, r)
        w_go(i, 15 + n, axes(i)[5], shard(i, order(i)[r], wrap(axes(i)[1] + 1, 4), half))

    def got_fwd_up(i, n):
        r, half = forwards(i)[0][n]
        w_got(i, 12 + n, shard(i, order(i)[r], wrap(axes(i)[1] + 2, 4), half))

    def got_fwd_dn(i, n):
        r, half = forwards(i)[1][n]
        w_got(i, 15 + n, shard(i, order(i)[r], wrap(axes(i)[1] + 2, 4), half))

    def share(i, k, region):
        w_go(i, k, other, region(core))

    def shared(i, k, region):
        w_got(i, k, region(1 - core))

    def row(i, n):
        sec = wrap(axes(i)[1] + (0, -1, 1)[n], 4)
        ref = items[i][0]
        return lambda cc: ref.at[cc, sec] if items[i][2] else ref.at[cc, :, sec]

    def single(i, r, step):
        f, sec = order(i)[r], wrap(axes(i)[1] + step, 4)
        return lambda cc: shard(i, f, sec, None, cc)

    def share_row(i, n):
        share(i, 18 + n, row(i, n))

    def share_far(i, r):
        share(i, 21 + r, single(i, r, 2))

    def all_shared(i):
        for n in range(3):
            shared(i, 18 + n, row(i, n))
        for r in (0, 2, 1, 3):
            shared(i, 21 + r, single(i, r, 2))

    def own_down(cc):
        return wd.at[cc, :, x]

    def share_down(r, n):
        share(DOWN, 19 + 3 * r + n, single(DOWN, r, (-1, 1, 2)[n]))

    def down_shared(r):
        for n in range(3):
            shared(DOWN, 19 + 3 * r + n, single(DOWN, r, (-1, 1, 2)[n]))

    for i in (GATE, UP, DOWN):
        w_copies[i].wait()
        step1(i)
    for i in (GATE, UP):
        across_up(i, 0)
        across_dn(i, 0)

    ones = jnp.ones((8, 128), F32)

    def ps_copy(c, d, owner):
        return remote(
            pst.at[owner, :, pl.ds(c * CT, CT)], ps_send.at[c, d], ps_recv.at[c, d], z_peers[d]
        )

    for c in range(CHUNKS):
        st_copies[c].wait()
        tok = pl.ds(c * CT, CT)
        squares = jnp.zeros((CT, COLS), F32)
        raw = jnp.zeros((24, CT), F32)
        for k in range(STREAMS):
            v = st[k, tok, :]
            squares = squares + v * v
            raw = raw + nt_dot(mw[:, k, :], v)
        squares = (squares[:, :128] + squares[:, 128:256]) + (squares[:, 256:384] + squares[:, 384:])
        sq_row = nt_dot(ones, squares, lax.Precision.HIGHEST)
        pst[z, 0:4, tok] = raw[0:4]
        pst[z, 4:8, tok] = sq_row[4:8]
        ost[z, 0:20, tok] = raw[4:24]
        ost[z, 20:24, tok] = sq_row[4:8]
        for d in far_first:
            cp = ps_copy(c, d, z)
            cp.start()
            sends.append(cp)

    def hops(c, to_right):
        return 4 if (c % 2 == 0) == to_right else 3

    def ag_copy(c, h, to_right, origin):
        q = 0 if to_right else 1
        return remote(
            xg.at[origin, pl.ds(c * CT, CT), :], ag_send.at[q, c, h], ag_recv.at[q, c, h],
            right if to_right else left,
        )

    def ag_go(c, h, to_right, origin):
        cp = ag_copy(c, h, to_right, origin)
        cp.start()
        sends.append(cp)

    row8 = lax.broadcasted_iota(jnp.int32, (8, 1), 0)
    bias8 = jnp.zeros((8, 1), F32)
    for l in range(4):
        bias8 = jnp.where(row8 == l, bias[l], bias8)
    g_row = jnp.concatenate([g32[pl.ds(4 * z + q, 1), :] for q in range(4)], axis=1)

    def layer_input(c):
        tok = pl.ds(c * CT, CT)
        for d in far_first:
            ps_copy(c, d, wrap(z - d, NZ)).wait_recv()
        total = pst[0, :, tok]
        for o in range(1, NZ):
            total = total + pst[o, :, tok]
        inverse = lax.rsqrt(total[4:5] / float(STREAMS * COLS * NZ) + EPSILON)
        pre = jax.nn.sigmoid(scale[0] * (total * inverse) + bias8)
        pre = jnp.concatenate([pre, jnp.zeros((120, CT), F32)], axis=0)
        pre_t[tok, :] = pre.T
        layer_in = pre_t[tok, 0:1] * st[0, tok, :]
        for k in range(1, STREAMS):
            layer_in = layer_in + pre_t[tok, k : k + 1] * st[k, tok, :]
        sent = (layer_in * g_row).astype(BF16)
        for q in range(4):
            xg[z, tok, q * 128 : (q + 1) * 128] = sent[:, PERM[q] * 128 : (PERM[q] + 1) * 128]
        ag_go(c, 0, True, z)
        ag_go(c, 0, False, z)
        sq = layer_in * layer_in
        sq = (sq[:, :128] + sq[:, 128:256]) + (sq[:, 256:384] + sq[:, 384:])
        sqx[z, :, tok] = nt_dot(ones, sq, lax.Precision.HIGHEST)[0:1]

    for c in range(CHUNKS):
        layer_input(c)

    def ag_step(h, chunks):
        for c in chunks:
            for to_right in (True, False):
                if h < hops(c, to_right):
                    origin = wrap(z - (h + 1), NZ) if to_right else wrap(z + (h + 1), NZ)
                    ag_copy(c, h, to_right, origin).wait_recv()
                    if h + 1 < hops(c, to_right):
                        ag_go(c, h + 1, to_right, origin)

    for i in (GATE, UP):
        step2(i)
    for i in (UP, GATE):
        across_up(i, 1)
        across_dn(i, 2)
        across_up(i, 2)
        across_dn(i, 1)
    for d in far_first:
        cp = remote(sqx.at[z], sq_send.at[d], sq_recv.at[d], z_peers[d])
        cp.start()
        sends.append(cp)
    ag_step(0, (0, 1))
    step2(DOWN)
    ag_step(0, (2, 3))
    for i in (UP, GATE):
        step2_end(i)
        across_up(i, 3)
        across_dn(i, 3)
        share_row(i, 0)
    ag_step(1, (0, 1))
    fwd_up(UP, 0)
    fwd_up(UP, 1)
    fwd_dn(UP, 0)
    ag_step(1, (2, 3))
    fwd_dn(UP, 1)
    step2_end(DOWN)
    share(DOWN, 18, own_down)
    for up, dn in ((0, 1), (1, 0)):
        across_up(DOWN, up)
        across_dn(DOWN, dn)
    fwd_up(GATE, 0)
    fwd_up(GATE, 1)
    fwd_dn(GATE, 0)
    got_up(UP, 2)
    got_up(UP, 3)
    share_row(UP, 1)
    got_dn(UP, 0)
    got_dn(UP, 1)
    share_row(UP, 2)
    ag_step(2, (0, 1))
    got_fwd_up(UP, 0)
    share_far(UP, 0)
    got_fwd_dn(UP, 0)
    share_far(UP, 2)
    ag_step(2, (2,))
    fwd_dn(GATE, 1)
    got_up(GATE, 2)
    got_up(GATE, 3)
    share_row(GATE, 1)
    got_dn(GATE, 0)
    got_dn(GATE, 1)
    share_row(GATE, 2)
    ag_step(2, (3,))
    for d in far_first:
        cp = remote(ost.at[z], os_send.at[d], os_recv.at[d], z_peers[d])
        cp.start()
        sends.append(cp)
    got_fwd_up(UP, 1)
    share_far(UP, 1)
    got_fwd_dn(UP, 1)
    share_far(UP, 3)
    for d in far_first:
        remote(sqx.at[wrap(z - d, NZ)], sq_send.at[d], sq_recv.at[d], z_peers[d]).wait_recv()
    sq_total = sqx[0]
    for o in range(1, NZ):
        sq_total = sq_total + sqx[o]
    inv = lax.rsqrt(sq_total / float(COLS * NZ) + EPSILON)
    inv_t[...] = jnp.broadcast_to(inv, (128, TOK)).T
    ag_step(3, (0,))
    got_fwd_up(GATE, 0)
    share_far(GATE, 0)
    got_fwd_dn(GATE, 0)
    share_far(GATE, 2)
    fwd_up(DOWN, 0)
    fwd_dn(DOWN, 0)
    send_halves(2)
    share_down(0, 0)
    share_down(1, 1)
    ag_step(3, (1,))
    got_fwd_up(GATE, 1)
    share_far(GATE, 1)
    got_fwd_dn(GATE, 1)
    share_far(GATE, 3)
    all_shared(UP)
    all_shared(GATE)

    halves = 2
    ht = TOK // halves

    def gate_up(half, first, last):
        def tile(n, carry):
            tok = pl.ds(half * ht, ht)
            lanes = pl.ds(pl.multiple_of(n * 128, 128), 128)
            acc = None
            for b in range(NZ):
                for cc in range(2):
                    a = xg[b, tok, cc * 256 : (cc + 1) * 256]
                    j = 2 * (b % 2)
                    bg = wg[cc, b // 2, j : j + 2, :, lanes].reshape(256, 128)
                    bu = wu[cc, b // 2, j : j + 2, :, lanes].reshape(256, 128)
                    d = jnp.dot(a, jnp.concatenate([bg, bu], axis=1), preferred_element_type=F32)
                    acc = d if acc is None else acc + d
            scale_t = inv_t[tok, :]
            g = acc[:, :128] * scale_t
            u = acc[:, 128:] * scale_t
            hid[tok, lanes] = (g / (1.0 + jnp.exp(-g)) * u).astype(BF16)
            return carry

        lax.fori_loop(first, last, tile, 0)

    def partial(dest, tok):
        a = hid[tok, :]
        parts = []
        j = 2 * lax.rem(dest, 2)
        for cc in range(2):
            b0 = wd[cc, lax.div(dest, 2), j]
            b1 = wd[cc, lax.div(dest, 2), j + 1]
            parts.append(
                jnp.dot(a, jnp.concatenate([b0, b1], axis=1), preferred_element_type=F32)
            )
        return parts

    def rs_copy(q, c, t):
        src, dst = (sr, rr) if q == 0 else (sl, rl)
        return pltpu.make_async_remote_copy(
            src_ref=src.at[c, t], dst_ref=dst.at[c, t],
            send_sem=rs_send.at[q, c, t], recv_sem=rs_recv.at[q, c, t],
            device_id=right if q == 0 else left, device_id_type=MESH,
        )

    def rs_step(t, first, last):
        def chunk(c, carry):
            odd = lax.rem(c, 2)
            tok = pl.ds(pl.multiple_of(c * CT, CT), CT)
            for q in range(2):
                n_hops = 4 - odd if q == 0 else 3 + odd

                def send():
                    dest = wrap(z + n_hops - t, NZ) if q == 0 else wrap(z - n_hops + t, NZ)
                    p0, p1 = partial(dest, tok)
                    src, dst = (sr, rr) if q == 0 else (sl, rl)
                    if t == 0:
                        src[c, t, :, 0:256] = p0.astype(BF16)
                        src[c, t, :, 256:512] = p1.astype(BF16)
                    else:
                        tmp[:, 0:256] = p0
                        tmp[:, 256:512] = p1
                        rs_copy(q, c, t - 1).wait_recv()
                        src[c, t] = (tmp[...] + dst[c, t - 1].astype(F32)).astype(BF16)
                    rs_copy(q, c, t).start()

                if t < 3:
                    send()
                else:
                    pl.when(n_hops == 4)(send)
            return carry

        lax.fori_loop(first, last, chunk, 0)

    gate_up(0, 0, 5)
    got_up(DOWN, 1)
    share_down(1, 0)
    got_dn(DOWN, 0)
    share_down(0, 1)
    gate_up(0, 5, 6)
    got_fwd_up(DOWN, 0)
    share_down(0, 2)
    got_fwd_dn(DOWN, 0)
    share_down(1, 2)
    gate_up(0, 6, 7)
    ag_step(3, (2, 3))
    gate_up(1, 0, 1)
    fwd_half_up(2)
    fwd_half_dn(2)
    send_halves(3)
    shared(DOWN, 18, own_down)
    down_shared(0)
    down_shared(1)
    rs_step(0, 0, 2)
    gate_up(1, 1, 4)
    got_half_up(2, 1)
    share_down(2, 0)
    got_half_dn(2, 0)
    share_down(2, 1)
    gate_up(1, 4, 7)
    rs_step(0, 2, 4)
    fwd_half_up(3)
    fwd_half_dn(3)
    got_fwd_up(DOWN, 1)
    got_fwd_dn(DOWN, 1)
    share_down(2, 2)
    down_shared(2)
    rs_step(1, 0, 4)
    got_half_up(3, 1)
    share_down(3, 0)
    got_half_dn(3, 0)
    share_down(3, 1)
    got_fwd_up(DOWN, 2)
    got_fwd_dn(DOWN, 2)
    share_down(3, 2)
    down_shared(3)

    for d in far_first:
        remote(ost.at[wrap(z - d, NZ)], os_send.at[d], os_recv.at[d], z_peers[d]).wait_recv()
    total = pst[0]
    rest = ost[0]
    for o in range(1, NZ):
        total = total + pst[o]
        rest = rest + ost[o]
    rest = rest * lax.rsqrt(total[4:5] / float(STREAMS * COLS * NZ) + EPSILON)
    row4 = lax.broadcasted_iota(jnp.int32, (4, 1), 0)

    def bias4(first):
        b = jnp.full((4, 1), bias[first], F32)
        for l in range(1, 4):
            b = jnp.where(row4 == l, bias[first + l], b)
        return b

    post = 2.0 * jax.nn.sigmoid(scale[1] * rest[0:4] + bias4(4))
    mix = tuple(
        jnp.exp(scale[2] * rest[4 + 4 * k : 8 + 4 * k] + bias4(8 + 4 * k)) for k in range(4)
    )

    def balance(_, m):
        m = tuple(v / jnp.sum(v, axis=0, keepdims=True) for v in m)
        col = (m[0] + m[1]) + (m[2] + m[3])
        return tuple(v / col for v in m)

    mix = lax.fori_loop(0, SWEEPS, balance, mix)
    coef = jnp.concatenate((post,) + mix + (jnp.zeros((108, TOK), F32),), axis=0)
    coef_t[...] = coef.T

    rs_step(2, 0, 4)
    for c in sends:
        c.wait_send()
    rs_step(3, 0, 4)

    def out_body(c, carry):
        odd = lax.rem(c, 2)
        tok = pl.ds(pl.multiple_of(c * CT, CT), CT)
        p0, p1 = partial(z, tok)
        tmp[:, 0:256] = p0
        tmp[:, 256:512] = p1
        rs_copy(0, c, 3 - odd).wait_recv()
        rs_copy(1, c, 2 + odd).wait_recv()
        tmp[...] = (
            tmp[...] + rr[c, 3 - odd].astype(F32) + rl[c, 2 + odd].astype(F32)
        )
        for q in range(4):
            lo[tok, PERM[q] * 128 : (PERM[q] + 1) * 128] = tmp[:, q * 128 : (q + 1) * 128]
        return carry

    lax.fori_loop(0, CHUNKS, out_body, 0)

    for c in range(CHUNKS):
        for q in range(2):
            for t in range(hops(c, q == 0)):
                rs_copy(q, c, t).wait_send()


def mix_kernel(st_hbm, lo_hbm, coef_hbm, out_hbm, st, lo, coef_t, out, in_sem, out_sem):
    def tokens(c):
        return pl.ds(c * CT, CT)

    def reads(c):
        return (
            pltpu.make_async_copy(coef_hbm.at[tokens(c)], coef_t.at[tokens(c)], in_sem.at[c, 0]),
            pltpu.make_async_copy(lo_hbm.at[tokens(c)], lo.at[tokens(c)], in_sem.at[c, 1]),
            pltpu.make_async_copy(st_hbm.at[:, tokens(c)], st.at[:, tokens(c)], in_sem.at[c, 2]),
        )

    def write(c):
        return pltpu.make_async_copy(out.at[:, tokens(c)], out_hbm.at[:, tokens(c)], out_sem.at[c])

    for c in range(CHUNKS):
        for copy in reads(c):
            copy.start()
    rows = 16

    for c in range(CHUNKS):
        for copy in reads(c):
            copy.wait()

        def group(g, carry):
            tok = pl.ds(pl.multiple_of(c * CT + g * rows, rows), rows)
            wide = [
                jnp.broadcast_to(coef_t[tok, n : n + 1], (rows, 128)) for n in range(5 * STREAMS)
            ]
            for q in range(COLS // 128):
                lanes = slice(q * 128, (q + 1) * 128)
                low = lo[tok, lanes]
                src = [st[j, tok, lanes] for j in range(STREAMS)]
                for k in range(STREAMS):
                    v = wide[k] * low
                    for j in range(STREAMS):
                        v = v + wide[STREAMS + STREAMS * k + j] * src[j]
                    out[k, tok, lanes] = v
            return carry

        lax.fori_loop(0, CT // rows, group, 0)
        write(c).start()
    for c in range(CHUNKS):
        write(c).wait()


def body(streams, mix_weight, mix_bias, mix_scale, norm_gain, gate_weight, up_weight, down_weight):
    gain = norm_gain.reshape(NZ * 4, 128)
    hbm = pl.BlockSpec(memory_space=pltpu.HBM)
    vmem = pl.BlockSpec(memory_space=pltpu.VMEM)
    smem = pl.BlockSpec(memory_space=pltpu.SMEM)
    dma = pltpu.SemaphoreType.DMA
    layer_out, coef = pl.pallas_call(
        kernel,
        out_shape=(
            jax.ShapeDtypeStruct((TOK, COLS), F32),
            jax.ShapeDtypeStruct((TOK, 128), F32),
        ),
        in_specs=[hbm, vmem, smem, smem, vmem, hbm, hbm, hbm],
        out_specs=(vmem, vmem),
        scratch_shapes=[
            pltpu.VMEM((STREAMS, TOK, COLS), F32),
            pltpu.VMEM((2, NY, NX, ROWS, FFL), BF16),
            pltpu.VMEM((2, NY, NX, ROWS, FFL), BF16),
            pltpu.VMEM((2, NY, NX, FFL, 128), BF16),
            pltpu.VMEM((NZ, TOK, COLS), BF16),
            pltpu.VMEM((TOK, FFL), BF16),
            pltpu.VMEM((CHUNKS, 4, CT, COLS), BF16),
            pltpu.VMEM((CHUNKS, 4, CT, COLS), BF16),
            pltpu.VMEM((CHUNKS, 4, CT, COLS), BF16),
            pltpu.VMEM((CHUNKS, 4, CT, COLS), BF16),
            pltpu.VMEM((NZ, 8, TOK), F32),
            pltpu.VMEM((NZ, 24, TOK), F32),
            pltpu.VMEM((NZ, 1, TOK), F32),
            pltpu.VMEM((TOK, 128), F32),
            pltpu.VMEM((TOK, 128), F32),
            pltpu.VMEM((CT, COLS), F32),
            pltpu.VMEM((NZ * 4, 128), F32),
            dma((CHUNKS + 3,)),
            dma((3, 36)),
            dma((3, 36)),
            dma((2, CHUNKS, 4)),
            dma((2, CHUNKS, 4)),
            dma((2, CHUNKS, 4)),
            dma((2, CHUNKS, 4)),
            dma((CHUNKS, 8)),
            dma((CHUNKS, 8)),
            dma((8,)),
            dma((8,)),
            dma((8,)),
            dma((8,)),
        ],
        compiler_params=pltpu.CompilerParams(
            collective_id=0, has_side_effects=True, vmem_limit_bytes=60 * 1024 * 1024
        ),
    )(streams, mix_weight, mix_bias, mix_scale, gain, gate_weight, up_weight, down_weight)
    return pl.pallas_call(
        mix_kernel,
        out_shape=jax.ShapeDtypeStruct((STREAMS, TOK, COLS), F32),
        in_specs=[hbm, hbm, hbm],
        out_specs=hbm,
        scratch_shapes=[
            pltpu.VMEM((STREAMS, TOK, COLS), F32),
            pltpu.VMEM((TOK, COLS), F32),
            pltpu.VMEM((TOK, 128), F32),
            pltpu.VMEM((STREAMS, TOK, COLS), F32),
            dma((CHUNKS, 3)),
            dma((CHUNKS,)),
        ],
        compiler_params=pltpu.CompilerParams(vmem_limit_bytes=60 * 1024 * 1024),
    )(streams, layer_out, coef)


def solution(mesh):
    placed = (
        P(None, "seq", "tensor"),
        P(None, None, "tensor"),
        P(),
        P(),
        P(),
        P("seq", "tensor"),
        P("seq", "tensor"),
        P("tensor", "seq"),
    )
    return jax.shard_map(
        body, mesh=mesh, in_specs=placed, out_specs=P(None, "seq", "tensor"), check_vma=False
    )
```

```python
import functools

import jax
import jax.numpy as jnp
from jax import lax
from jax.experimental import pallas as pl
from jax.experimental.pallas import tpu as pltpu
from jax.sharding import PartitionSpec as P

STREAMS = 4
SWEEPS = 20
EPSILON = 0.25
MESH = pl.DeviceIdType.MESH
NX = 4
NY = 4
NZ = 8
TOK = 512
COLS = 512
ROWS = 128
FFL = 896
CHUNKS = 4
CT = TOK // CHUNKS
MT = 64
PERM = (0, 2, 1, 3)
F32 = jnp.float32
BF16 = jnp.bfloat16


def wrap(value, size):
    return lax.rem(value + size, size)


def nt_dot(a, b, precision=None):
    return lax.dot_general(
        a, b, (((1,), (1,)), ((), ())), precision=precision, preferred_element_type=F32
    )


def kernel(
    st_hbm, mw, bias, scale, gain, g_hbm, u_hbm, d_hbm, base_hbm, lo_hbm, post_hbm,
    st, wg, wu, wd, xg, hid, rr, rl, sr, sl, pst, ost, sqx, pre_t, inv_t, tmp, g32,
    base, lo, own, coef_t, loc_sem, out_sem, w_send, w_recv, ag_send, ag_recv, rs_send, rs_recv,
    ps_send, ps_recv, os_send, os_recv, sq_send, sq_recv,
):
    s = lax.axis_index("seq")
    z = lax.axis_index("tensor")
    core = lax.rem(s, 2)
    x = lax.rem(lax.div(s, 2), NX)
    y = lax.div(s, 2 * NX)

    def at(xx, yy, cc):
        return {"seq": (yy * NX + xx) * 2 + cc, "tensor": z}

    x_up, x_dn = at(wrap(x + 1, NX), y, core), at(wrap(x - 1, NX), y, core)
    y_up, y_dn = at(x, wrap(y + 1, NY), core), at(x, wrap(y - 1, NY), core)
    other = at(x, y, 1 - core)
    right = {"seq": s, "tensor": wrap(z + 1, NZ)}
    left = {"seq": s, "tensor": wrap(z - 1, NZ)}
    z_peers = {d: {"seq": s, "tensor": wrap(z + d, NZ)} for d in range(1, NZ)}
    far_first = (4, 3, 5, 2, 6, 1, 7)

    w_copies = [
        pltpu.make_async_copy(src, dst.at[core, y, x], loc_sem.at[CHUNKS + i])
        for i, (src, dst) in enumerate(((g_hbm, wg), (u_hbm, wu), (d_hbm, wd)))
    ]
    st_copies = [
        pltpu.make_async_copy(
            st_hbm.at[:, pl.ds(c * CT, CT), :], st.at[:, pl.ds(c * CT, CT), :], loc_sem.at[c]
        )
        for c in range(CHUNKS)
    ]
    for c in w_copies + st_copies:
        c.start()

    barrier = pltpu.get_barrier_semaphore()
    peers = [x_up, x_dn, y_up, y_dn, other] + [z_peers[d] for d in range(1, NZ)]
    for peer in peers:
        pl.semaphore_signal(barrier, inc=1, device_id=peer, device_id_type=MESH)
    g32[...] = gain[...].astype(F32)
    pl.semaphore_wait(barrier, len(peers))

    sends = []

    def remote(ref, send_sem, recv_sem, dev):
        return pltpu.make_async_remote_copy(
            src_ref=ref, dst_ref=ref, send_sem=send_sem, recv_sem=recv_sem,
            device_id=dev, device_id_type=MESH,
        )

    GATE, UP, DOWN = 0, 1, 2
    items = ((wg, ROWS, True), (wu, ROWS, False), (wd, FFL, False))

    def axes(i):
        if items[i][2]:
            return x, y, x_up, x_dn, y_up, y_dn
        return y, x, y_up, y_dn, x_up, x_dn

    def shard(i, f, sec, half=None, cc=None):
        ref, rows, x_first = items[i]
        cc = core if cc is None else cc
        rsl = slice(None) if half is None else pl.ds(half * (rows // 2), rows // 2)
        return ref.at[cc, sec, f, rsl, :] if x_first else ref.at[cc, f, sec, rsl, :]

    def w_copy(i, k, dev, region):
        return remote(region, w_send.at[i, k], w_recv.at[i, k], dev)

    def w_go(i, k, dev, region):
        c = w_copy(i, k, dev, region)
        c.start()
        sends.append(c)

    def w_got(i, k, region):
        w_copy(i, k, other, region).wait_recv()

    zq = lax.div(z, 2)
    zo = lax.rem(z, 2)
    need = [wrap(zq + 2, 4), wrap(zq + 1 + 2 * zo, 4), wrap(zq + 3 - 2 * zo, 4), wrap(zq, 4)]

    def order(i):
        f = axes(i)[0]
        if i == DOWN:
            return need
        return [f, wrap(f - 1, 4), wrap(f + 1, 4), wrap(f + 2, 4)]

    def forwards(i):
        if i == DOWN:
            return ((0, None), (2, 0), (3, 0)), ((1, None), (2, 1), (3, 1))
        return ((0, None), (1, None)), ((2, None), (3, None))

    def step1(i):
        f, sec, f_up, f_dn, _, _ = axes(i)
        w_go(i, 0, f_up, shard(i, f, sec))
        w_go(i, 1, f_dn, shard(i, f, sec))

    def step2(i):
        f, sec, f_up, f_dn, _, _ = axes(i)
        fm, fp = wrap(f - 1, 4), wrap(f + 1, 4)
        w_got(i, 0, shard(i, fm, sec))
        w_go(i, 2, f_up, shard(i, fm, sec, 0))
        w_got(i, 1, shard(i, fp, sec))
        w_go(i, 3, f_dn, shard(i, fp, sec, 1))

    def step2_end(i):
        f, sec = axes(i)[:2]
        w_got(i, 2, shard(i, wrap(f + 2, 4), sec, 0))
        w_got(i, 3, shard(i, wrap(f + 2, 4), sec, 1))

    def half_up(r, n):
        k = 4 + r if n == 0 else 30 + r
        w_go(DOWN, k, axes(DOWN)[4], shard(DOWN, need[r], x, n))

    def half_dn(r, n):
        k = 8 + r if n == 1 else 32 + r
        w_go(DOWN, k, axes(DOWN)[5], shard(DOWN, need[r], x, n))

    def got_half_up(r, n):
        w_got(DOWN, 4 + r if n == 0 else 30 + r, shard(DOWN, need[r], wrap(x - 1, 4), n))

    def got_half_dn(r, n):
        w_got(DOWN, 8 + r if n == 1 else 32 + r, shard(DOWN, need[r], wrap(x + 1, 4), n))

    def fwd_half_up(r):
        got_half_up(r, 0)
        w_go(DOWN, 11 + r, axes(DOWN)[4], shard(DOWN, need[r], wrap(x - 1, 4), 0))

    def fwd_half_dn(r):
        got_half_dn(r, 1)
        w_go(DOWN, 14 + r, axes(DOWN)[5], shard(DOWN, need[r], wrap(x + 1, 4), 1))

    def send_halves(r):
        half_up(r, 0)
        half_dn(r, 1)
        half_up(r, 1)
        half_dn(r, 0)

    def across_up(i, r):
        w_go(i, 4 + r, axes(i)[4], shard(i, order(i)[r], axes(i)[1]))

    def across_dn(i, r):
        w_go(i, 8 + r, axes(i)[5], shard(i, order(i)[r], axes(i)[1]))

    def got_up(i, r):
        w_got(i, 4 + r, shard(i, order(i)[r], wrap(axes(i)[1] - 1, 4)))

    def got_dn(i, r):
        w_got(i, 8 + r, shard(i, order(i)[r], wrap(axes(i)[1] + 1, 4)))

    def fwd_up(i, n):
        r, half = forwards(i)[0][n]
        if n == 0 or forwards(i)[0][n - 1][0] != r:
            got_up(i, r)
        w_go(i, 12 + n, axes(i)[4], shard(i, order(i)[r], wrap(axes(i)[1] - 1, 4), half))

    def fwd_dn(i, n):
        r, half = forwards(i)[1][n]
        got_dn(i, r)
        w_go(i, 15 + n, axes(i)[5], shard(i, order(i)[r], wrap(axes(i)[1] + 1, 4), half))

    def got_fwd_up(i, n):
        r, half = forwards(i)[0][n]
        w_got(i, 12 + n, shard(i, order(i)[r], wrap(axes(i)[1] + 2, 4), half))

    def got_fwd_dn(i, n):
        r, half = forwards(i)[1][n]
        w_got(i, 15 + n, shard(i, order(i)[r], wrap(axes(i)[1] + 2, 4), half))

    def share(i, k, region):
        w_go(i, k, other, region(core))

    def shared(i, k, region):
        w_got(i, k, region(1 - core))

    def row(i, n):
        sec = wrap(axes(i)[1] + (0, -1, 1)[n], 4)
        ref = items[i][0]
        return lambda cc: ref.at[cc, sec] if items[i][2] else ref.at[cc, :, sec]

    def single(i, r, step):
        f, sec = order(i)[r], wrap(axes(i)[1] + step, 4)
        return lambda cc: shard(i, f, sec, None, cc)

    def share_row(i, n):
        share(i, 18 + n, row(i, n))

    def share_far(i, r):
        share(i, 21 + r, single(i, r, 2))

    def all_shared(i):
        for n in range(3):
            shared(i, 18 + n, row(i, n))
        for r in (0, 2, 1, 3):
            shared(i, 21 + r, single(i, r, 2))

    def own_down(cc):
        return wd.at[cc, :, x]

    def share_down(r, n):
        share(DOWN, 19 + 3 * r + n, single(DOWN, r, (-1, 1, 2)[n]))

    def down_shared(r):
        for n in range(3):
            shared(DOWN, 19 + 3 * r + n, single(DOWN, r, (-1, 1, 2)[n]))

    for i in (GATE, UP, DOWN):
        w_copies[i].wait()
        step1(i)
    for i in (GATE, UP):
        across_up(i, 0)
        across_dn(i, 0)

    ones = jnp.ones((8, 128), F32)

    def ps_copy(c, d, owner):
        return remote(
            pst.at[owner, :, pl.ds(c * CT, CT)], ps_send.at[c, d], ps_recv.at[c, d], z_peers[d]
        )

    for c in range(CHUNKS):
        st_copies[c].wait()
        tok = pl.ds(c * CT, CT)
        squares = jnp.zeros((CT, COLS), F32)
        raw = jnp.zeros((24, CT), F32)
        for k in range(STREAMS):
            v = st[k, tok, :]
            squares = squares + v * v
            raw = raw + nt_dot(mw[:, k, :], v)
        squares = (squares[:, :128] + squares[:, 128:256]) + (squares[:, 256:384] + squares[:, 384:])
        sq_row = nt_dot(ones, squares, lax.Precision.HIGHEST)
        pst[z, 0:4, tok] = raw[0:4]
        pst[z, 4:8, tok] = sq_row[4:8]
        ost[z, 0:20, tok] = raw[4:24]
        ost[z, 20:24, tok] = sq_row[4:8]
        for d in far_first:
            cp = ps_copy(c, d, z)
            cp.start()
            sends.append(cp)

    def hops(c, to_right):
        return 4 if (c % 2 == 0) == to_right else 3

    def ag_copy(c, h, to_right, origin):
        q = 0 if to_right else 1
        return remote(
            xg.at[origin, pl.ds(c * CT, CT), :], ag_send.at[q, c, h], ag_recv.at[q, c, h],
            right if to_right else left,
        )

    def ag_go(c, h, to_right, origin):
        cp = ag_copy(c, h, to_right, origin)
        cp.start()
        sends.append(cp)

    row8 = lax.broadcasted_iota(jnp.int32, (8, 1), 0)
    bias8 = jnp.zeros((8, 1), F32)
    for l in range(4):
        bias8 = jnp.where(row8 == l, bias[l], bias8)
    g_row = jnp.concatenate([g32[pl.ds(4 * z + q, 1), :] for q in range(4)], axis=1)

    def layer_input(c):
        tok = pl.ds(c * CT, CT)
        for d in far_first:
            ps_copy(c, d, wrap(z - d, NZ)).wait_recv()
        total = pst[0, :, tok]
        for o in range(1, NZ):
            total = total + pst[o, :, tok]
        inverse = lax.rsqrt(total[4:5] / float(STREAMS * COLS * NZ) + EPSILON)
        pre = jax.nn.sigmoid(scale[0] * (total * inverse) + bias8)
        pre = jnp.concatenate([pre, jnp.zeros((120, CT), F32)], axis=0)
        pre_t[tok, :] = pre.T
        layer_in = pre_t[tok, 0:1] * st[0, tok, :]
        for k in range(1, STREAMS):
            layer_in = layer_in + pre_t[tok, k : k + 1] * st[k, tok, :]
        sent = (layer_in * g_row).astype(BF16)
        for q in range(4):
            xg[z, tok, q * 128 : (q + 1) * 128] = sent[:, PERM[q] * 128 : (PERM[q] + 1) * 128]
        ag_go(c, 0, True, z)
        ag_go(c, 0, False, z)
        sq = layer_in * layer_in
        sq = (sq[:, :128] + sq[:, 128:256]) + (sq[:, 256:384] + sq[:, 384:])
        sqx[z, :, tok] = nt_dot(ones, sq, lax.Precision.HIGHEST)[0:1]

    for c in range(CHUNKS):
        layer_input(c)

    def ag_step(h, chunks):
        for c in chunks:
            for to_right in (True, False):
                if h < hops(c, to_right):
                    origin = wrap(z - (h + 1), NZ) if to_right else wrap(z + (h + 1), NZ)
                    ag_copy(c, h, to_right, origin).wait_recv()
                    if h + 1 < hops(c, to_right):
                        ag_go(c, h + 1, to_right, origin)

    for i in (GATE, UP):
        step2(i)
    for i in (UP, GATE):
        across_up(i, 1)
        across_dn(i, 2)
        across_up(i, 2)
        across_dn(i, 1)
    for d in far_first:
        cp = remote(sqx.at[z], sq_send.at[d], sq_recv.at[d], z_peers[d])
        cp.start()
        sends.append(cp)
    ag_step(0, (0, 1))
    step2(DOWN)
    ag_step(0, (2, 3))
    for i in (UP, GATE):
        step2_end(i)
        across_up(i, 3)
        across_dn(i, 3)
        share_row(i, 0)
    ag_step(1, (0, 1))
    fwd_up(UP, 0)
    fwd_up(UP, 1)
    fwd_dn(UP, 0)
    ag_step(1, (2, 3))
    fwd_dn(UP, 1)
    step2_end(DOWN)
    share(DOWN, 18, own_down)
    for up, dn in ((0, 1), (1, 0)):
        across_up(DOWN, up)
        across_dn(DOWN, dn)
    fwd_up(GATE, 0)
    fwd_up(GATE, 1)
    fwd_dn(GATE, 0)
    got_up(UP, 2)
    got_up(UP, 3)
    share_row(UP, 1)
    got_dn(UP, 0)
    got_dn(UP, 1)
    share_row(UP, 2)
    ag_step(2, (0, 1))
    got_fwd_up(UP, 0)
    share_far(UP, 0)
    got_fwd_dn(UP, 0)
    share_far(UP, 2)
    ag_step(2, (2,))
    fwd_dn(GATE, 1)
    got_up(GATE, 2)
    got_up(GATE, 3)
    share_row(GATE, 1)
    got_dn(GATE, 0)
    got_dn(GATE, 1)
    share_row(GATE, 2)
    ag_step(2, (3,))
    for d in far_first:
        cp = remote(ost.at[z], os_send.at[d], os_recv.at[d], z_peers[d])
        cp.start()
        sends.append(cp)
    got_fwd_up(UP, 1)
    share_far(UP, 1)
    got_fwd_dn(UP, 1)
    share_far(UP, 3)
    for d in far_first:
        remote(sqx.at[wrap(z - d, NZ)], sq_send.at[d], sq_recv.at[d], z_peers[d]).wait_recv()
    sq_total = sqx[0]
    for o in range(1, NZ):
        sq_total = sq_total + sqx[o]
    inv = lax.rsqrt(sq_total / float(COLS * NZ) + EPSILON)
    inv_t[...] = jnp.broadcast_to(inv, (128, TOK)).T
    ag_step(3, (0,))
    got_fwd_up(GATE, 0)
    share_far(GATE, 0)
    got_fwd_dn(GATE, 0)
    share_far(GATE, 2)
    fwd_up(DOWN, 0)
    fwd_dn(DOWN, 0)
    send_halves(2)
    share_down(0, 0)
    share_down(1, 1)
    ag_step(3, (1,))
    got_fwd_up(GATE, 1)
    share_far(GATE, 1)
    got_fwd_dn(GATE, 1)
    share_far(GATE, 3)
    all_shared(UP)
    all_shared(GATE)

    halves = 2
    ht = TOK // halves

    def gate_up(half, first, last):
        def tile(n, carry):
            tok = pl.ds(half * ht, ht)
            lanes = pl.ds(pl.multiple_of(n * 128, 128), 128)
            acc = None
            for b in range(NZ):
                for cc in range(2):
                    a = xg[b, tok, cc * 256 : (cc + 1) * 256]
                    j = 2 * (b % 2)
                    bg = wg[cc, b // 2, j : j + 2, :, lanes].reshape(256, 128)
                    bu = wu[cc, b // 2, j : j + 2, :, lanes].reshape(256, 128)
                    d = jnp.dot(a, jnp.concatenate([bg, bu], axis=1), preferred_element_type=F32)
                    acc = d if acc is None else acc + d
            scale_t = inv_t[tok, :]
            g = acc[:, :128] * scale_t
            u = acc[:, 128:] * scale_t
            hid[tok, lanes] = (g / (1.0 + jnp.exp(-g)) * u).astype(BF16)
            return carry

        lax.fori_loop(first, last, tile, 0)

    def partial(dest, tok):
        a = hid[tok, :]
        parts = []
        j = 2 * lax.rem(dest, 2)
        for cc in range(2):
            b0 = wd[cc, lax.div(dest, 2), j]
            b1 = wd[cc, lax.div(dest, 2), j + 1]
            parts.append(
                jnp.dot(a, jnp.concatenate([b0, b1], axis=1), preferred_element_type=F32)
            )
        return parts

    def rs_copy(q, c, t):
        src, dst = (sr, rr) if q == 0 else (sl, rl)
        return pltpu.make_async_remote_copy(
            src_ref=src.at[c, t], dst_ref=dst.at[c, t],
            send_sem=rs_send.at[q, c, t], recv_sem=rs_recv.at[q, c, t],
            device_id=right if q == 0 else left, device_id_type=MESH,
        )

    def rs_step(t, first, last):
        def chunk(c, carry):
            odd = lax.rem(c, 2)
            tok = pl.ds(pl.multiple_of(c * CT, CT), CT)
            for q in range(2):
                n_hops = 4 - odd if q == 0 else 3 + odd

                def send():
                    dest = wrap(z + n_hops - t, NZ) if q == 0 else wrap(z - n_hops + t, NZ)
                    p0, p1 = partial(dest, tok)
                    src, dst = (sr, rr) if q == 0 else (sl, rl)
                    if t == 0:
                        src[c, t, :, 0:256] = p0.astype(BF16)
                        src[c, t, :, 256:512] = p1.astype(BF16)
                    else:
                        tmp[:, 0:256] = p0
                        tmp[:, 256:512] = p1
                        rs_copy(q, c, t - 1).wait_recv()
                        src[c, t] = (tmp[...] + dst[c, t - 1].astype(F32)).astype(BF16)
                    rs_copy(q, c, t).start()

                if t < 3:
                    send()
                else:
                    pl.when(n_hops == 4)(send)
            return carry

        lax.fori_loop(first, last, chunk, 0)

    gate_up(0, 0, 7)
    got_up(DOWN, 1)
    share_down(1, 0)
    got_dn(DOWN, 0)
    share_down(0, 1)
    ag_step(3, (2, 3))
    got_fwd_up(DOWN, 0)
    share_down(0, 2)
    got_fwd_dn(DOWN, 0)
    share_down(1, 2)
    gate_up(1, 0, 1)
    shared(DOWN, 18, own_down)
    down_shared(0)
    down_shared(1)
    rs_step(0, 0, 2)
    fwd_half_up(2)
    fwd_half_dn(2)
    send_halves(3)
    gate_up(1, 1, 4)
    got_half_up(2, 1)
    share_down(2, 0)
    got_half_dn(2, 0)
    share_down(2, 1)
    gate_up(1, 4, 7)
    rs_step(0, 2, 4)
    fwd_half_up(3)
    fwd_half_dn(3)
    got_fwd_up(DOWN, 1)
    got_fwd_dn(DOWN, 1)
    share_down(2, 2)
    down_shared(2)
    rs_step(1, 0, 4)
    got_half_up(3, 1)
    share_down(3, 0)
    got_half_dn(3, 0)
    share_down(3, 1)
    got_fwd_up(DOWN, 2)
    got_fwd_dn(DOWN, 2)
    share_down(3, 2)
    down_shared(3)

    for d in far_first:
        remote(ost.at[wrap(z - d, NZ)], os_send.at[d], os_recv.at[d], z_peers[d]).wait_recv()
    total = pst[0]
    rest = ost[0]
    for o in range(1, NZ):
        total = total + pst[o]
        rest = rest + ost[o]
    rest = rest * lax.rsqrt(total[4:5] / float(STREAMS * COLS * NZ) + EPSILON)
    row4 = lax.broadcasted_iota(jnp.int32, (4, 1), 0)

    def bias4(first):
        b = jnp.full((4, 1), bias[first], F32)
        for l in range(1, 4):
            b = jnp.where(row4 == l, bias[first + l], b)
        return b

    post = 2.0 * jax.nn.sigmoid(scale[1] * rest[0:4] + bias4(4))
    mix = tuple(
        jnp.exp(scale[2] * rest[4 + 4 * k : 8 + 4 * k] + bias4(8 + 4 * k)) for k in range(4)
    )

    def balance(_, m):
        m = tuple(v / jnp.sum(v, axis=0, keepdims=True) for v in m)
        col = (m[0] + m[1]) + (m[2] + m[3])
        return tuple(v / col for v in m)

    mix = lax.fori_loop(0, SWEEPS, balance, mix)
    coef = jnp.concatenate((post,) + mix + (jnp.zeros((108, TOK), F32),), axis=0)
    coef_t[...] = coef.T

    def post_write():
        return pltpu.make_async_copy(coef_t, post_hbm, out_sem.at[2 * CHUNKS])

    def base_write(c):
        tok = pl.ds(pl.multiple_of(c * CT, CT), CT)
        return pltpu.make_async_copy(base.at[:, tok, :], base_hbm.at[:, tok, :], out_sem.at[c])

    def lo_write(c):
        tok = pl.ds(pl.multiple_of(c * CT, CT), CT)
        return pltpu.make_async_copy(lo.at[tok, :], lo_hbm.at[tok, :], out_sem.at[CHUNKS + c])

    def residual(c):
        rows = 16

        def group(g, carry):
            tok = pl.ds(pl.multiple_of(c * CT + g * rows, rows), rows)
            wide = [
                jnp.broadcast_to(coef_t[tok, STREAMS + n : STREAMS + n + 1], (rows, 128))
                for n in range(STREAMS * STREAMS)
            ]
            for q in range(COLS // 128):
                lanes = slice(q * 128, (q + 1) * 128)
                src = [st[j, tok, lanes] for j in range(STREAMS)]
                for k in range(STREAMS):
                    v = wide[STREAMS * k] * src[0]
                    for j in range(1, STREAMS):
                        v = v + wide[STREAMS * k + j] * src[j]
                    base[k, tok, lanes] = v
            return carry

        lax.fori_loop(0, CT // rows, group, 0)
        base_write(c).start()

    post_write().start()
    residual(0)
    rs_step(2, 0, 2)
    residual(1)
    rs_step(2, 2, 4)
    for c in sends:
        c.wait_send()
    residual(2)
    rs_step(3, 0, 2)
    residual(3)
    rs_step(3, 2, 4)

    def own_body(c, carry):
        tok = pl.ds(pl.multiple_of(c * CT, CT), CT)
        p0, p1 = partial(z, tok)
        own[tok, 0:256] = p0
        own[tok, 256:512] = p1
        return carry

    lax.fori_loop(0, CHUNKS, own_body, 0)

    def out_body(c, carry):
        odd = lax.rem(c, 2)
        tok = pl.ds(pl.multiple_of(c * CT, CT), CT)
        rs_copy(0, c, 3 - odd).wait_recv()
        rs_copy(1, c, 2 + odd).wait_recv()
        for q in range(4):
            lanes = slice(q * 128, (q + 1) * 128)
            lo[tok, PERM[q] * 128 : (PERM[q] + 1) * 128] = (
                own[tok, lanes]
                + rr[c, 3 - odd, :, lanes].astype(F32)
                + rl[c, 2 + odd, :, lanes].astype(F32)
            )
        lo_write(c).start()
        return carry

    lax.fori_loop(0, CHUNKS, out_body, 0)

    for c in range(CHUNKS):
        for q in range(2):
            for t in range(hops(c, q == 0)):
                rs_copy(q, c, t).wait_send()
    post_write().wait()
    for c in range(CHUNKS):
        base_write(c).wait()
        lo_write(c).wait()


def mix_kernel(base_hbm, lo_hbm, post_hbm, out_hbm, base, lo, post, in_sem, out_sem):
    def tokens(c):
        return pl.ds(c * MT, MT)

    def reads(c):
        return (
            pltpu.make_async_copy(post_hbm.at[tokens(c)], post.at[tokens(c)], in_sem.at[c, 0]),
            pltpu.make_async_copy(lo_hbm.at[tokens(c)], lo.at[tokens(c)], in_sem.at[c, 1]),
            pltpu.make_async_copy(base_hbm.at[:, tokens(c)], base.at[:, tokens(c)], in_sem.at[c, 2]),
        )

    def write(c):
        return pltpu.make_async_copy(base.at[:, tokens(c)], out_hbm.at[:, tokens(c)], out_sem.at[c])

    for c in range(TOK // MT):
        for copy in reads(c):
            copy.start()
    for c in range(TOK // MT):
        for copy in reads(c):
            copy.wait()
        tok = slice(c * MT, (c + 1) * MT)
        for k in range(STREAMS):
            base[k, tok, :] = base[k, tok, :] + post[tok, k : k + 1] * lo[tok, :]
        write(c).start()
    for c in range(TOK // MT):
        write(c).wait()


def body(streams, mix_weight, mix_bias, mix_scale, norm_gain, gate_weight, up_weight, down_weight):
    gain = norm_gain.reshape(NZ * 4, 128)
    hbm = pl.BlockSpec(memory_space=pltpu.HBM)
    vmem = pl.BlockSpec(memory_space=pltpu.VMEM)
    smem = pl.BlockSpec(memory_space=pltpu.SMEM)
    dma = pltpu.SemaphoreType.DMA
    base, layer_out, post = pl.pallas_call(
        kernel,
        out_shape=(
            jax.ShapeDtypeStruct((STREAMS, TOK, COLS), F32),
            jax.ShapeDtypeStruct((TOK, COLS), F32),
            jax.ShapeDtypeStruct((TOK, 128), F32),
        ),
        in_specs=[hbm, vmem, smem, smem, vmem, hbm, hbm, hbm],
        out_specs=(hbm, hbm, hbm),
        scratch_shapes=[
            pltpu.VMEM((STREAMS, TOK, COLS), F32),
            pltpu.VMEM((2, NY, NX, ROWS, FFL), BF16),
            pltpu.VMEM((2, NY, NX, ROWS, FFL), BF16),
            pltpu.VMEM((2, NY, NX, FFL, 128), BF16),
            pltpu.VMEM((NZ, TOK, COLS), BF16),
            pltpu.VMEM((TOK, FFL), BF16),
            pltpu.VMEM((CHUNKS, 4, CT, COLS), BF16),
            pltpu.VMEM((CHUNKS, 4, CT, COLS), BF16),
            pltpu.VMEM((CHUNKS, 4, CT, COLS), BF16),
            pltpu.VMEM((CHUNKS, 4, CT, COLS), BF16),
            pltpu.VMEM((NZ, 8, TOK), F32),
            pltpu.VMEM((NZ, 24, TOK), F32),
            pltpu.VMEM((NZ, 1, TOK), F32),
            pltpu.VMEM((TOK, 128), F32),
            pltpu.VMEM((TOK, 128), F32),
            pltpu.VMEM((CT, COLS), F32),
            pltpu.VMEM((NZ * 4, 128), F32),
            pltpu.VMEM((STREAMS, TOK, COLS), F32),
            pltpu.VMEM((TOK, COLS), F32),
            pltpu.VMEM((TOK, COLS), F32),
            pltpu.VMEM((TOK, 128), F32),
            dma((CHUNKS + 3,)),
            dma((2 * CHUNKS + 1,)),
            dma((3, 36)),
            dma((3, 36)),
            dma((2, CHUNKS, 4)),
            dma((2, CHUNKS, 4)),
            dma((2, CHUNKS, 4)),
            dma((2, CHUNKS, 4)),
            dma((CHUNKS, 8)),
            dma((CHUNKS, 8)),
            dma((8,)),
            dma((8,)),
            dma((8,)),
            dma((8,)),
        ],
        compiler_params=pltpu.CompilerParams(
            collective_id=0, has_side_effects=True, vmem_limit_bytes=60 * 1024 * 1024
        ),
    )(streams, mix_weight, mix_bias, mix_scale, gain, gate_weight, up_weight, down_weight)
    return pl.pallas_call(
        mix_kernel,
        out_shape=jax.ShapeDtypeStruct((STREAMS, TOK, COLS), F32),
        in_specs=[hbm, hbm, hbm],
        out_specs=hbm,
        scratch_shapes=[
            pltpu.VMEM((STREAMS, TOK, COLS), F32),
            pltpu.VMEM((TOK, COLS), F32),
            pltpu.VMEM((TOK, 128), F32),
            dma((TOK // MT, 3)),
            dma((TOK // MT,)),
        ],
        compiler_params=pltpu.CompilerParams(vmem_limit_bytes=60 * 1024 * 1024),
    )(base, layer_out, post)


def solution(mesh):
    placed = (
        P(None, "seq", "tensor"),
        P(None, None, "tensor"),
        P(),
        P(),
        P(),
        P("seq", "tensor"),
        P("seq", "tensor"),
        P("tensor", "seq"),
    )
    return jax.shard_map(
        body, mesh=mesh, in_specs=placed, out_specs=P(None, "seq", "tensor"), check_vma=False
    )
```

```python
import functools

import jax
import jax.numpy as jnp
from jax import lax
from jax.experimental import pallas as pl
from jax.experimental.pallas import tpu as pltpu
from jax.sharding import PartitionSpec as P

STREAMS = 4
SWEEPS = 20
EPSILON = 0.25
MESH = pl.DeviceIdType.MESH
NX = 4
NY = 4
NZ = 8
TOK = 512
COLS = 512
ROWS = 128
FFL = 896
CHUNKS = 4
CT = TOK // CHUNKS
MT = 64
PERM = (0, 2, 1, 3)
F32 = jnp.float32
BF16 = jnp.bfloat16


def wrap(value, size):
    return lax.rem(value + size, size)


def nt_dot(a, b, precision=None):
    return lax.dot_general(
        a, b, (((1,), (1,)), ((), ())), precision=precision, preferred_element_type=F32
    )


def kernel(
    st_hbm, mw_hbm, bias_hbm, scale_hbm, gain_hbm, g_hbm, u_hbm, d_hbm, base_hbm, lo_hbm, post_hbm,
    st, wg, wu, wd, xg, hid, rr, rl, sr, sl, pst, ost, sqx, pre_t, inv_t, tmp, g32,
    base, lo, own, coef_t, mw, bias, scale, gain, loc_sem, out_sem, w_send, w_recv, ag_send, ag_recv, rs_send, rs_recv,
    ps_send, ps_recv, os_send, os_recv, sq_send, sq_recv,
):
    s = lax.axis_index("seq")
    z = lax.axis_index("tensor")
    core = lax.rem(s, 2)
    x = lax.rem(lax.div(s, 2), NX)
    y = lax.div(s, 2 * NX)

    def at(xx, yy, cc):
        return {"seq": (yy * NX + xx) * 2 + cc, "tensor": z}

    x_up, x_dn = at(wrap(x + 1, NX), y, core), at(wrap(x - 1, NX), y, core)
    y_up, y_dn = at(x, wrap(y + 1, NY), core), at(x, wrap(y - 1, NY), core)
    other = at(x, y, 1 - core)
    right = {"seq": s, "tensor": wrap(z + 1, NZ)}
    left = {"seq": s, "tensor": wrap(z - 1, NZ)}
    z_peers = {d: {"seq": s, "tensor": wrap(z + d, NZ)} for d in range(1, NZ)}
    far_first = (4, 3, 5, 2, 6, 1, 7)

    w_copies = [
        pltpu.make_async_copy(src, dst.at[core, y, x], loc_sem.at[CHUNKS + i])
        for i, (src, dst) in enumerate(((g_hbm, wg), (u_hbm, wu), (d_hbm, wd)))
    ]
    st_copies = [
        pltpu.make_async_copy(
            st_hbm.at[:, pl.ds(c * CT, CT), :], st.at[:, pl.ds(c * CT, CT), :], loc_sem.at[c]
        )
        for c in range(CHUNKS)
    ]
    small = [
        pltpu.make_async_copy(src, dst, loc_sem.at[CHUNKS + 3 + i])
        for i, (src, dst) in enumerate(
            ((mw_hbm, mw), (gain_hbm, gain), (scale_hbm, scale), (bias_hbm, bias))
        )
    ]
    for c in w_copies + small + st_copies:
        c.start()

    barrier = pltpu.get_barrier_semaphore()
    peers = [x_up, x_dn, y_up, y_dn, other] + [z_peers[d] for d in range(1, NZ)]
    for peer in peers:
        pl.semaphore_signal(barrier, inc=1, device_id=peer, device_id_type=MESH)
    pl.semaphore_wait(barrier, len(peers))

    sends = []

    def remote(ref, send_sem, recv_sem, dev):
        return pltpu.make_async_remote_copy(
            src_ref=ref, dst_ref=ref, send_sem=send_sem, recv_sem=recv_sem,
            device_id=dev, device_id_type=MESH,
        )

    GATE, UP, DOWN = 0, 1, 2
    items = ((wg, ROWS, True), (wu, ROWS, False), (wd, FFL, False))

    def axes(i):
        if items[i][2]:
            return x, y, x_up, x_dn, y_up, y_dn
        return y, x, y_up, y_dn, x_up, x_dn

    def shard(i, f, sec, half=None, cc=None):
        ref, rows, x_first = items[i]
        cc = core if cc is None else cc
        rsl = slice(None) if half is None else pl.ds(half * (rows // 2), rows // 2)
        return ref.at[cc, sec, f, rsl, :] if x_first else ref.at[cc, f, sec, rsl, :]

    def w_copy(i, k, dev, region):
        return remote(region, w_send.at[i, k], w_recv.at[i, k], dev)

    def w_go(i, k, dev, region):
        c = w_copy(i, k, dev, region)
        c.start()
        sends.append(c)

    def w_got(i, k, region):
        w_copy(i, k, other, region).wait_recv()

    zq = lax.div(z, 2)
    zo = lax.rem(z, 2)
    need = [wrap(zq + 2, 4), wrap(zq + 1 + 2 * zo, 4), wrap(zq + 3 - 2 * zo, 4), wrap(zq, 4)]

    def order(i):
        f = axes(i)[0]
        if i == DOWN:
            return need
        return [f, wrap(f - 1, 4), wrap(f + 1, 4), wrap(f + 2, 4)]

    def forwards(i):
        if i == DOWN:
            return ((0, None), (2, 0), (3, 0)), ((1, None), (2, 1), (3, 1))
        return ((0, None), (1, None)), ((2, None), (3, None))

    def step1(i):
        f, sec, f_up, f_dn, _, _ = axes(i)
        w_go(i, 0, f_up, shard(i, f, sec))
        w_go(i, 1, f_dn, shard(i, f, sec))

    def step2(i):
        f, sec, f_up, f_dn, _, _ = axes(i)
        fm, fp = wrap(f - 1, 4), wrap(f + 1, 4)
        w_got(i, 0, shard(i, fm, sec))
        w_go(i, 2, f_up, shard(i, fm, sec, 0))
        w_got(i, 1, shard(i, fp, sec))
        w_go(i, 3, f_dn, shard(i, fp, sec, 1))

    def step2_end(i):
        f, sec = axes(i)[:2]
        w_got(i, 2, shard(i, wrap(f + 2, 4), sec, 0))
        w_got(i, 3, shard(i, wrap(f + 2, 4), sec, 1))

    def half_up(r, n):
        k = 4 + r if n == 0 else 30 + r
        w_go(DOWN, k, axes(DOWN)[4], shard(DOWN, need[r], x, n))

    def half_dn(r, n):
        k = 8 + r if n == 1 else 32 + r
        w_go(DOWN, k, axes(DOWN)[5], shard(DOWN, need[r], x, n))

    def got_half_up(r, n):
        w_got(DOWN, 4 + r if n == 0 else 30 + r, shard(DOWN, need[r], wrap(x - 1, 4), n))

    def got_half_dn(r, n):
        w_got(DOWN, 8 + r if n == 1 else 32 + r, shard(DOWN, need[r], wrap(x + 1, 4), n))

    def fwd_half_up(r):
        got_half_up(r, 0)
        w_go(DOWN, 11 + r, axes(DOWN)[4], shard(DOWN, need[r], wrap(x - 1, 4), 0))

    def fwd_half_dn(r):
        got_half_dn(r, 1)
        w_go(DOWN, 14 + r, axes(DOWN)[5], shard(DOWN, need[r], wrap(x + 1, 4), 1))

    def send_halves(r):
        half_up(r, 0)
        half_dn(r, 1)
        half_up(r, 1)
        half_dn(r, 0)

    def across_up(i, r):
        w_go(i, 4 + r, axes(i)[4], shard(i, order(i)[r], axes(i)[1]))

    def across_dn(i, r):
        w_go(i, 8 + r, axes(i)[5], shard(i, order(i)[r], axes(i)[1]))

    def got_up(i, r):
        w_got(i, 4 + r, shard(i, order(i)[r], wrap(axes(i)[1] - 1, 4)))

    def got_dn(i, r):
        w_got(i, 8 + r, shard(i, order(i)[r], wrap(axes(i)[1] + 1, 4)))

    def fwd_up(i, n):
        r, half = forwards(i)[0][n]
        if n == 0 or forwards(i)[0][n - 1][0] != r:
            got_up(i, r)
        w_go(i, 12 + n, axes(i)[4], shard(i, order(i)[r], wrap(axes(i)[1] - 1, 4), half))

    def fwd_dn(i, n):
        r, half = forwards(i)[1][n]
        got_dn(i, r)
        w_go(i, 15 + n, axes(i)[5], shard(i, order(i)[r], wrap(axes(i)[1] + 1, 4), half))

    def got_fwd_up(i, n):
        r, half = forwards(i)[0][n]
        w_got(i, 12 + n, shard(i, order(i)[r], wrap(axes(i)[1] + 2, 4), half))

    def got_fwd_dn(i, n):
        r, half = forwards(i)[1][n]
        w_got(i, 15 + n, shard(i, order(i)[r], wrap(axes(i)[1] + 2, 4), half))

    def share(i, k, region):
        w_go(i, k, other, region(core))

    def shared(i, k, region):
        w_got(i, k, region(1 - core))

    def row(i, n):
        sec = wrap(axes(i)[1] + (0, -1, 1)[n], 4)
        ref = items[i][0]
        return lambda cc: ref.at[cc, sec] if items[i][2] else ref.at[cc, :, sec]

    def single(i, r, step):
        f, sec = order(i)[r], wrap(axes(i)[1] + step, 4)
        return lambda cc: shard(i, f, sec, None, cc)

    def share_row(i, n):
        share(i, 18 + n, row(i, n))

    def share_far(i, r):
        share(i, 21 + r, single(i, r, 2))

    def all_shared(i):
        for n in range(3):
            shared(i, 18 + n, row(i, n))
        for r in (0, 2, 1, 3):
            shared(i, 21 + r, single(i, r, 2))

    def own_down(cc):
        return wd.at[cc, :, x]

    def share_down(r, n):
        share(DOWN, 19 + 3 * r + n, single(DOWN, r, (-1, 1, 2)[n]))

    def down_shared(r):
        for n in range(3):
            shared(DOWN, 19 + 3 * r + n, single(DOWN, r, (-1, 1, 2)[n]))

    for i in (GATE, UP, DOWN):
        w_copies[i].wait()
        step1(i)
    for i in (GATE, UP):
        across_up(i, 0)
        across_dn(i, 0)

    ones = jnp.ones((8, 128), F32)
    for c in small:
        c.wait()
    g32[...] = gain[...].astype(F32)

    def ps_copy(c, d, owner):
        return remote(
            pst.at[owner, :, pl.ds(c * CT, CT)], ps_send.at[c, d], ps_recv.at[c, d], z_peers[d]
        )

    for c in range(CHUNKS):
        st_copies[c].wait()
        tok = pl.ds(c * CT, CT)
        squares = jnp.zeros((CT, COLS), F32)
        raw = jnp.zeros((24, CT), F32)
        for k in range(STREAMS):
            v = st[k, tok, :]
            squares = squares + v * v
            raw = raw + nt_dot(mw[:, k, :], v)
        squares = (squares[:, :128] + squares[:, 128:256]) + (squares[:, 256:384] + squares[:, 384:])
        sq_row = nt_dot(ones, squares, lax.Precision.HIGHEST)
        pst[z, 0:4, tok] = raw[0:4]
        pst[z, 4:8, tok] = sq_row[4:8]
        ost[z, 0:20, tok] = raw[4:24]
        ost[z, 20:24, tok] = sq_row[4:8]
        for d in far_first:
            cp = ps_copy(c, d, z)
            cp.start()
            sends.append(cp)

    def hops(c, to_right):
        return 4 if (c % 2 == 0) == to_right else 3

    def ag_copy(c, h, to_right, origin):
        q = 0 if to_right else 1
        return remote(
            xg.at[origin, pl.ds(c * CT, CT), :], ag_send.at[q, c, h], ag_recv.at[q, c, h],
            right if to_right else left,
        )

    def ag_go(c, h, to_right, origin):
        cp = ag_copy(c, h, to_right, origin)
        cp.start()
        sends.append(cp)

    row8 = lax.broadcasted_iota(jnp.int32, (8, 1), 0)
    bias8 = jnp.zeros((8, 1), F32)
    for l in range(4):
        bias8 = jnp.where(row8 == l, bias[l], bias8)
    g_row = jnp.concatenate([g32[pl.ds(4 * z + q, 1), :] for q in range(4)], axis=1)

    def layer_input(c):
        tok = pl.ds(c * CT, CT)
        for d in far_first:
            ps_copy(c, d, wrap(z - d, NZ)).wait_recv()
        total = pst[0, :, tok]
        for o in range(1, NZ):
            total = total + pst[o, :, tok]
        inverse = lax.rsqrt(total[4:5] / float(STREAMS * COLS * NZ) + EPSILON)
        pre = jax.nn.sigmoid(scale[0] * (total * inverse) + bias8)
        pre = jnp.concatenate([pre, jnp.zeros((120, CT), F32)], axis=0)
        pre_t[tok, :] = pre.T
        layer_in = pre_t[tok, 0:1] * st[0, tok, :]
        for k in range(1, STREAMS):
            layer_in = layer_in + pre_t[tok, k : k + 1] * st[k, tok, :]
        sent = (layer_in * g_row).astype(BF16)
        for q in range(4):
            xg[z, tok, q * 128 : (q + 1) * 128] = sent[:, PERM[q] * 128 : (PERM[q] + 1) * 128]
        ag_go(c, 0, True, z)
        ag_go(c, 0, False, z)
        sq = layer_in * layer_in
        sq = (sq[:, :128] + sq[:, 128:256]) + (sq[:, 256:384] + sq[:, 384:])
        sqx[z, :, tok] = nt_dot(ones, sq, lax.Precision.HIGHEST)[0:1]

    for c in range(CHUNKS):
        layer_input(c)

    def ag_step(h, chunks):
        for c in chunks:
            for to_right in (True, False):
                if h < hops(c, to_right):
                    origin = wrap(z - (h + 1), NZ) if to_right else wrap(z + (h + 1), NZ)
                    ag_copy(c, h, to_right, origin).wait_recv()
                    if h + 1 < hops(c, to_right):
                        ag_go(c, h + 1, to_right, origin)

    for i in (GATE, UP):
        step2(i)
    for i in (UP, GATE):
        across_up(i, 1)
        across_dn(i, 2)
        across_up(i, 2)
        across_dn(i, 1)
    for d in far_first:
        cp = remote(sqx.at[z], sq_send.at[d], sq_recv.at[d], z_peers[d])
        cp.start()
        sends.append(cp)
    ag_step(0, (0, 1))
    step2(DOWN)
    ag_step(0, (2, 3))
    for i in (UP, GATE):
        step2_end(i)
        across_up(i, 3)
        across_dn(i, 3)
        share_row(i, 0)
    ag_step(1, (0, 1))
    fwd_up(UP, 0)
    fwd_up(UP, 1)
    fwd_dn(UP, 0)
    ag_step(1, (2, 3))
    fwd_dn(UP, 1)
    step2_end(DOWN)
    share(DOWN, 18, own_down)
    for up, dn in ((0, 1), (1, 0)):
        across_up(DOWN, up)
        across_dn(DOWN, dn)
    fwd_up(GATE, 0)
    fwd_up(GATE, 1)
    fwd_dn(GATE, 0)
    got_up(UP, 2)
    got_up(UP, 3)
    share_row(UP, 1)
    got_dn(UP, 0)
    got_dn(UP, 1)
    share_row(UP, 2)
    ag_step(2, (0, 1))
    got_fwd_up(UP, 0)
    share_far(UP, 0)
    got_fwd_dn(UP, 0)
    share_far(UP, 2)
    ag_step(2, (2,))
    fwd_dn(GATE, 1)
    got_up(GATE, 2)
    got_up(GATE, 3)
    share_row(GATE, 1)
    got_dn(GATE, 0)
    got_dn(GATE, 1)
    share_row(GATE, 2)
    ag_step(2, (3,))
    for d in far_first:
        cp = remote(ost.at[z], os_send.at[d], os_recv.at[d], z_peers[d])
        cp.start()
        sends.append(cp)
    got_fwd_up(UP, 1)
    share_far(UP, 1)
    got_fwd_dn(UP, 1)
    share_far(UP, 3)
    for d in far_first:
        remote(sqx.at[wrap(z - d, NZ)], sq_send.at[d], sq_recv.at[d], z_peers[d]).wait_recv()
    sq_total = sqx[0]
    for o in range(1, NZ):
        sq_total = sq_total + sqx[o]
    inv = lax.rsqrt(sq_total / float(COLS * NZ) + EPSILON)
    inv_t[...] = jnp.broadcast_to(inv, (128, TOK)).T
    ag_step(3, (0,))
    got_fwd_up(GATE, 0)
    share_far(GATE, 0)
    got_fwd_dn(GATE, 0)
    share_far(GATE, 2)
    fwd_up(DOWN, 0)
    fwd_dn(DOWN, 0)
    send_halves(2)
    share_down(0, 0)
    share_down(1, 1)
    ag_step(3, (1,))
    got_fwd_up(GATE, 1)
    share_far(GATE, 1)
    got_fwd_dn(GATE, 1)
    share_far(GATE, 3)
    all_shared(UP)
    all_shared(GATE)

    halves = 2
    ht = TOK // halves

    def gate_up(half, first, last):
        def tile(n, carry):
            tok = pl.ds(half * ht, ht)
            lanes = pl.ds(pl.multiple_of(n * 128, 128), 128)
            acc = None
            for b in range(NZ):
                for cc in range(2):
                    a = xg[b, tok, cc * 256 : (cc + 1) * 256]
                    j = 2 * (b % 2)
                    bg = wg[cc, b // 2, j : j + 2, :, lanes].reshape(256, 128)
                    bu = wu[cc, b // 2, j : j + 2, :, lanes].reshape(256, 128)
                    d = jnp.dot(a, jnp.concatenate([bg, bu], axis=1), preferred_element_type=F32)
                    acc = d if acc is None else acc + d
            scale_t = inv_t[tok, :]
            g = acc[:, :128] * scale_t
            u = acc[:, 128:] * scale_t
            hid[tok, lanes] = (g / (1.0 + jnp.exp(-g)) * u).astype(BF16)
            return carry

        lax.fori_loop(first, last, tile, 0)

    def partial(dest, tok):
        a = hid[tok, :]
        parts = []
        j = 2 * lax.rem(dest, 2)
        for cc in range(2):
            b0 = wd[cc, lax.div(dest, 2), j]
            b1 = wd[cc, lax.div(dest, 2), j + 1]
            parts.append(
                jnp.dot(a, jnp.concatenate([b0, b1], axis=1), preferred_element_type=F32)
            )
        return parts

    def rs_copy(q, c, t):
        src, dst = (sr, rr) if q == 0 else (sl, rl)
        return pltpu.make_async_remote_copy(
            src_ref=src.at[c, t], dst_ref=dst.at[c, t],
            send_sem=rs_send.at[q, c, t], recv_sem=rs_recv.at[q, c, t],
            device_id=right if q == 0 else left, device_id_type=MESH,
        )

    def rs_step(t, first, last):
        def chunk(c, carry):
            odd = lax.rem(c, 2)
            tok = pl.ds(pl.multiple_of(c * CT, CT), CT)
            for q in range(2):
                n_hops = 4 - odd if q == 0 else 3 + odd

                def send():
                    dest = wrap(z + n_hops - t, NZ) if q == 0 else wrap(z - n_hops + t, NZ)
                    p0, p1 = partial(dest, tok)
                    src, dst = (sr, rr) if q == 0 else (sl, rl)
                    if t == 0:
                        src[c, t, :, 0:256] = p0.astype(BF16)
                        src[c, t, :, 256:512] = p1.astype(BF16)
                    else:
                        tmp[:, 0:256] = p0
                        tmp[:, 256:512] = p1
                        rs_copy(q, c, t - 1).wait_recv()
                        src[c, t] = (tmp[...] + dst[c, t - 1].astype(F32)).astype(BF16)
                    rs_copy(q, c, t).start()

                if t < 3:
                    send()
                else:
                    pl.when(n_hops == 4)(send)
            return carry

        lax.fori_loop(first, last, chunk, 0)

    gate_up(0, 0, 7)
    got_up(DOWN, 1)
    share_down(1, 0)
    got_dn(DOWN, 0)
    share_down(0, 1)
    ag_step(3, (2, 3))
    got_fwd_up(DOWN, 0)
    share_down(0, 2)
    got_fwd_dn(DOWN, 0)
    share_down(1, 2)
    gate_up(1, 0, 1)
    shared(DOWN, 18, own_down)
    down_shared(0)
    down_shared(1)
    rs_step(0, 0, 2)
    fwd_half_up(2)
    fwd_half_dn(2)
    send_halves(3)
    gate_up(1, 1, 4)
    got_half_up(2, 1)
    share_down(2, 0)
    got_half_dn(2, 0)
    share_down(2, 1)
    gate_up(1, 4, 7)
    rs_step(0, 2, 4)
    got_fwd_up(DOWN, 1)
    got_fwd_dn(DOWN, 1)
    share_down(2, 2)
    fwd_half_up(3)
    fwd_half_dn(3)
    down_shared(2)
    rs_step(1, 0, 4)
    got_half_up(3, 1)
    share_down(3, 0)
    got_half_dn(3, 0)
    share_down(3, 1)
    got_fwd_up(DOWN, 2)
    got_fwd_dn(DOWN, 2)
    share_down(3, 2)
    down_shared(3)

    for d in far_first:
        remote(ost.at[wrap(z - d, NZ)], os_send.at[d], os_recv.at[d], z_peers[d]).wait_recv()
    total = pst[0]
    rest = ost[0]
    for o in range(1, NZ):
        total = total + pst[o]
        rest = rest + ost[o]
    rest = rest * lax.rsqrt(total[4:5] / float(STREAMS * COLS * NZ) + EPSILON)
    row4 = lax.broadcasted_iota(jnp.int32, (4, 1), 0)

    def bias4(first):
        b = jnp.full((4, 1), bias[first], F32)
        for l in range(1, 4):
            b = jnp.where(row4 == l, bias[first + l], b)
        return b

    post = 2.0 * jax.nn.sigmoid(scale[1] * rest[0:4] + bias4(4))
    mix = tuple(
        jnp.exp(scale[2] * rest[4 + 4 * k : 8 + 4 * k] + bias4(8 + 4 * k)) for k in range(4)
    )

    def balance(_, m):
        m = tuple(v / jnp.sum(v, axis=0, keepdims=True) for v in m)
        col = (m[0] + m[1]) + (m[2] + m[3])
        return tuple(v / col for v in m)

    mix = lax.fori_loop(0, SWEEPS, balance, mix)
    coef = jnp.concatenate((post,) + mix + (jnp.zeros((108, TOK), F32),), axis=0)
    coef_t[...] = coef.T

    def post_write():
        return pltpu.make_async_copy(coef_t, post_hbm, out_sem.at[2 * CHUNKS])

    def base_write(c):
        tok = pl.ds(pl.multiple_of(c * CT, CT), CT)
        return pltpu.make_async_copy(base.at[:, tok, :], base_hbm.at[:, tok, :], out_sem.at[c])

    def lo_write(c):
        tok = pl.ds(pl.multiple_of(c * CT, CT), CT)
        return pltpu.make_async_copy(lo.at[tok, :], lo_hbm.at[tok, :], out_sem.at[CHUNKS + c])

    def residual(c):
        rows = 16

        def group(g, carry):
            tok = pl.ds(pl.multiple_of(c * CT + g * rows, rows), rows)
            wide = [
                jnp.broadcast_to(coef_t[tok, STREAMS + n : STREAMS + n + 1], (rows, 128))
                for n in range(STREAMS * STREAMS)
            ]
            for q in range(COLS // 128):
                lanes = slice(q * 128, (q + 1) * 128)
                src = [st[j, tok, lanes] for j in range(STREAMS)]
                for k in range(STREAMS):
                    v = wide[STREAMS * k] * src[0]
                    for j in range(1, STREAMS):
                        v = v + wide[STREAMS * k + j] * src[j]
                    base[k, tok, lanes] = v.astype(BF16)
            return carry

        lax.fori_loop(0, CT // rows, group, 0)
        base_write(c).start()

    post_write().start()
    residual(0)
    rs_step(2, 0, 2)
    residual(1)
    rs_step(2, 2, 4)
    for c in sends:
        c.wait_send()
    residual(2)
    rs_step(3, 0, 2)
    residual(3)
    rs_step(3, 2, 4)

    def own_body(c, carry):
        tok = pl.ds(pl.multiple_of(c * CT, CT), CT)
        p0, p1 = partial(z, tok)
        own[tok, 0:256] = p0
        own[tok, 256:512] = p1
        return carry

    lax.fori_loop(0, CHUNKS, own_body, 0)

    def out_body(c, carry):
        odd = lax.rem(c, 2)
        tok = pl.ds(pl.multiple_of(c * CT, CT), CT)
        rs_copy(0, c, 3 - odd).wait_recv()
        rs_copy(1, c, 2 + odd).wait_recv()
        for q in range(4):
            lanes = slice(q * 128, (q + 1) * 128)
            lo[tok, PERM[q] * 128 : (PERM[q] + 1) * 128] = (
                own[tok, lanes]
                + rr[c, 3 - odd, :, lanes].astype(F32)
                + rl[c, 2 + odd, :, lanes].astype(F32)
            )
        lo_write(c).start()
        return carry

    lax.fori_loop(0, CHUNKS, out_body, 0)

    for c in range(CHUNKS):
        for q in range(2):
            for t in range(hops(c, q == 0)):
                rs_copy(q, c, t).wait_send()
    post_write().wait()
    for c in range(CHUNKS):
        base_write(c).wait()
        lo_write(c).wait()


def mix_kernel(base_hbm, lo_hbm, post_hbm, out_hbm, base, lo, post, out, in_sem, out_sem):
    def tokens(c):
        return pl.ds(c * MT, MT)

    def reads(c):
        return (
            pltpu.make_async_copy(post_hbm.at[tokens(c)], post.at[tokens(c)], in_sem.at[c, 0]),
            pltpu.make_async_copy(lo_hbm.at[tokens(c)], lo.at[tokens(c)], in_sem.at[c, 1]),
            pltpu.make_async_copy(base_hbm.at[:, tokens(c)], base.at[:, tokens(c)], in_sem.at[c, 2]),
        )

    def write(c):
        return pltpu.make_async_copy(out.at[:, tokens(c)], out_hbm.at[:, tokens(c)], out_sem.at[c])

    for c in range(TOK // MT):
        for copy in reads(c):
            copy.start()
    for c in range(TOK // MT):
        for copy in reads(c):
            copy.wait()
        tok = slice(c * MT, (c + 1) * MT)
        for k in range(STREAMS):
            out[k, tok, :] = base[k, tok, :].astype(F32) + post[tok, k : k + 1] * lo[tok, :]
        write(c).start()
    for c in range(TOK // MT):
        write(c).wait()


def body(streams, mix_weight, mix_bias, mix_scale, norm_gain, gate_weight, up_weight, down_weight):
    gain = norm_gain.reshape(NZ * 4, 128)
    hbm = pl.BlockSpec(memory_space=pltpu.HBM)
    dma = pltpu.SemaphoreType.DMA
    base, layer_out, post = pl.pallas_call(
        kernel,
        out_shape=(
            jax.ShapeDtypeStruct((STREAMS, TOK, COLS), BF16),
            jax.ShapeDtypeStruct((TOK, COLS), F32),
            jax.ShapeDtypeStruct((TOK, 128), F32),
        ),
        in_specs=[hbm] * 8,
        out_specs=(hbm, hbm, hbm),
        scratch_shapes=[
            pltpu.VMEM((STREAMS, TOK, COLS), F32),
            pltpu.VMEM((2, NY, NX, ROWS, FFL), BF16),
            pltpu.VMEM((2, NY, NX, ROWS, FFL), BF16),
            pltpu.VMEM((2, NY, NX, FFL, 128), BF16),
            pltpu.VMEM((NZ, TOK, COLS), BF16),
            pltpu.VMEM((TOK, FFL), BF16),
            pltpu.VMEM((CHUNKS, 4, CT, COLS), BF16),
            pltpu.VMEM((CHUNKS, 4, CT, COLS), BF16),
            pltpu.VMEM((CHUNKS, 4, CT, COLS), BF16),
            pltpu.VMEM((CHUNKS, 4, CT, COLS), BF16),
            pltpu.VMEM((NZ, 8, TOK), F32),
            pltpu.VMEM((NZ, 24, TOK), F32),
            pltpu.VMEM((NZ, 1, TOK), F32),
            pltpu.VMEM((TOK, 128), F32),
            pltpu.VMEM((TOK, 128), F32),
            pltpu.VMEM((CT, COLS), F32),
            pltpu.VMEM((NZ * 4, 128), F32),
            pltpu.VMEM((STREAMS, TOK, COLS), BF16),
            pltpu.VMEM((TOK, COLS), F32),
            pltpu.VMEM((TOK, COLS), F32),
            pltpu.VMEM((TOK, 128), F32),
            pltpu.VMEM((6 * STREAMS, STREAMS, COLS), F32),
            pltpu.SMEM((6 * STREAMS,), F32),
            pltpu.SMEM((3,), F32),
            pltpu.VMEM((NZ * 4, 128), BF16),
            dma((CHUNKS + 7,)),
            dma((2 * CHUNKS + 1,)),
            dma((3, 36)),
            dma((3, 36)),
            dma((2, CHUNKS, 4)),
            dma((2, CHUNKS, 4)),
            dma((2, CHUNKS, 4)),
            dma((2, CHUNKS, 4)),
            dma((CHUNKS, 8)),
            dma((CHUNKS, 8)),
            dma((8,)),
            dma((8,)),
            dma((8,)),
            dma((8,)),
        ],
        compiler_params=pltpu.CompilerParams(
            collective_id=0, has_side_effects=True, vmem_limit_bytes=60 * 1024 * 1024
        ),
    )(streams, mix_weight, mix_bias, mix_scale, gain, gate_weight, up_weight, down_weight)
    return pl.pallas_call(
        mix_kernel,
        out_shape=jax.ShapeDtypeStruct((STREAMS, TOK, COLS), F32),
        in_specs=[hbm, hbm, hbm],
        out_specs=hbm,
        scratch_shapes=[
            pltpu.VMEM((STREAMS, TOK, COLS), BF16),
            pltpu.VMEM((TOK, COLS), F32),
            pltpu.VMEM((TOK, 128), F32),
            pltpu.VMEM((STREAMS, TOK, COLS), F32),
            dma((TOK // MT, 3)),
            dma((TOK // MT,)),
        ],
        compiler_params=pltpu.CompilerParams(vmem_limit_bytes=60 * 1024 * 1024),
    )(base, layer_out, post)


def solution(mesh):
    placed = (
        P(None, "seq", "tensor"),
        P(None, None, "tensor"),
        P(),
        P(),
        P(),
        P("seq", "tensor"),
        P("seq", "tensor"),
        P("tensor", "seq"),
    )
    return jax.shard_map(
        body, mesh=mesh, in_specs=placed, out_specs=P(None, "seq", "tensor"), check_vma=False
    )
```

```python
import functools

import jax
import jax.numpy as jnp
from jax import lax
from jax.experimental import pallas as pl
from jax.experimental.pallas import tpu as pltpu
from jax.sharding import PartitionSpec as P

STREAMS = 4
SWEEPS = 20
EPSILON = 0.25
MESH = pl.DeviceIdType.MESH
NX = 4
NY = 4
NZ = 8
TOK = 512
COLS = 512
ROWS = 128
FFL = 896
CHUNKS = 4
CT = TOK // CHUNKS
MT = 64
PERM = (0, 2, 1, 3)
F32 = jnp.float32
BF16 = jnp.bfloat16


def wrap(value, size):
    return lax.rem(value + size, size)


def nt_dot(a, b, precision=None):
    return lax.dot_general(
        a, b, (((1,), (1,)), ((), ())), precision=precision, preferred_element_type=F32
    )


def kernel(
    st_hbm, mw_hbm, bias_hbm, scale_hbm, gain_hbm, g_hbm, u_hbm, d_hbm, base_hbm, lo_hbm, post_hbm,
    st, wg, wu, wd, xg, hid, rr, rl, sr, sl, pst, ost, sqx, pre_t, inv_t, tmp, g32,
    base, lo, own, coef_t, mw, bias, scale, gain, loc_sem, out_sem, w_send, w_recv, ag_send, ag_recv, rs_send, rs_recv,
    ps_send, ps_recv, os_send, os_recv, sq_send, sq_recv,
):
    s = lax.axis_index("seq")
    z = lax.axis_index("tensor")
    core = lax.rem(s, 2)
    x = lax.rem(lax.div(s, 2), NX)
    y = lax.div(s, 2 * NX)

    def at(xx, yy, cc):
        return {"seq": (yy * NX + xx) * 2 + cc, "tensor": z}

    x_up, x_dn = at(wrap(x + 1, NX), y, core), at(wrap(x - 1, NX), y, core)
    y_up, y_dn = at(x, wrap(y + 1, NY), core), at(x, wrap(y - 1, NY), core)
    other = at(x, y, 1 - core)
    right = {"seq": s, "tensor": wrap(z + 1, NZ)}
    left = {"seq": s, "tensor": wrap(z - 1, NZ)}
    z_peers = {d: {"seq": s, "tensor": wrap(z + d, NZ)} for d in range(1, NZ)}
    far_first = (4, 3, 5, 2, 6, 1, 7)

    w_copies = [
        pltpu.make_async_copy(src, dst.at[core, y, x], loc_sem.at[CHUNKS + i])
        for i, (src, dst) in enumerate(((g_hbm, wg), (u_hbm, wu), (d_hbm, wd)))
    ]
    st_copies = [
        pltpu.make_async_copy(
            st_hbm.at[:, pl.ds(c * CT, CT), :], st.at[:, pl.ds(c * CT, CT), :], loc_sem.at[c]
        )
        for c in range(CHUNKS)
    ]
    small = [
        pltpu.make_async_copy(src, dst, loc_sem.at[CHUNKS + 3 + i])
        for i, (src, dst) in enumerate(
            ((mw_hbm, mw), (gain_hbm, gain), (scale_hbm, scale), (bias_hbm, bias))
        )
    ]
    for c in w_copies + small + st_copies:
        c.start()

    barrier = pltpu.get_barrier_semaphore()
    peers = [x_up, x_dn, y_up, y_dn, other] + [z_peers[d] for d in range(1, NZ)]
    for peer in peers:
        pl.semaphore_signal(barrier, inc=1, device_id=peer, device_id_type=MESH)
    pl.semaphore_wait(barrier, len(peers))

    sends = []

    def remote(ref, send_sem, recv_sem, dev):
        return pltpu.make_async_remote_copy(
            src_ref=ref, dst_ref=ref, send_sem=send_sem, recv_sem=recv_sem,
            device_id=dev, device_id_type=MESH,
        )

    GATE, UP, DOWN = 0, 1, 2
    items = ((wg, ROWS, True), (wu, ROWS, False), (wd, FFL, False))

    def axes(i):
        if items[i][2]:
            return x, y, x_up, x_dn, y_up, y_dn
        return y, x, y_up, y_dn, x_up, x_dn

    def shard(i, f, sec, half=None, cc=None):
        ref, rows, x_first = items[i]
        cc = core if cc is None else cc
        rsl = slice(None) if half is None else pl.ds(half * (rows // 2), rows // 2)
        return ref.at[cc, sec, f, rsl, :] if x_first else ref.at[cc, f, sec, rsl, :]

    def w_copy(i, k, dev, region):
        return remote(region, w_send.at[i, k], w_recv.at[i, k], dev)

    def w_go(i, k, dev, region):
        c = w_copy(i, k, dev, region)
        c.start()
        sends.append(c)

    def w_got(i, k, region):
        w_copy(i, k, other, region).wait_recv()

    zq = lax.div(z, 2)
    zo = lax.rem(z, 2)
    need = [wrap(zq + 2, 4), wrap(zq + 1 + 2 * zo, 4), wrap(zq + 3 - 2 * zo, 4), wrap(zq, 4)]

    def order(i):
        f = axes(i)[0]
        if i == DOWN:
            return need
        return [f, wrap(f - 1, 4), wrap(f + 1, 4), wrap(f + 2, 4)]

    def forwards(i):
        if i == DOWN:
            return ((0, None), (2, 0), (3, 0)), ((1, None), (2, 1), (3, 1))
        return ((0, None), (1, None)), ((2, None), (3, None))

    def step1(i):
        f, sec, f_up, f_dn, _, _ = axes(i)
        w_go(i, 0, f_up, shard(i, f, sec))
        w_go(i, 1, f_dn, shard(i, f, sec))

    def step2(i):
        f, sec, f_up, f_dn, _, _ = axes(i)
        fm, fp = wrap(f - 1, 4), wrap(f + 1, 4)
        w_got(i, 0, shard(i, fm, sec))
        w_go(i, 2, f_up, shard(i, fm, sec, 0))
        w_got(i, 1, shard(i, fp, sec))
        w_go(i, 3, f_dn, shard(i, fp, sec, 1))

    def step2_end(i):
        f, sec = axes(i)[:2]
        w_got(i, 2, shard(i, wrap(f + 2, 4), sec, 0))
        w_got(i, 3, shard(i, wrap(f + 2, 4), sec, 1))

    def half_up(r, n):
        k = 4 + r if n == 0 else 30 + r
        w_go(DOWN, k, axes(DOWN)[4], shard(DOWN, need[r], x, n))

    def half_dn(r, n):
        k = 8 + r if n == 1 else 32 + r
        w_go(DOWN, k, axes(DOWN)[5], shard(DOWN, need[r], x, n))

    def got_half_up(r, n):
        w_got(DOWN, 4 + r if n == 0 else 30 + r, shard(DOWN, need[r], wrap(x - 1, 4), n))

    def got_half_dn(r, n):
        w_got(DOWN, 8 + r if n == 1 else 32 + r, shard(DOWN, need[r], wrap(x + 1, 4), n))

    def fwd_half_up(r):
        got_half_up(r, 0)
        w_go(DOWN, 11 + r, axes(DOWN)[4], shard(DOWN, need[r], wrap(x - 1, 4), 0))

    def fwd_half_dn(r):
        got_half_dn(r, 1)
        w_go(DOWN, 14 + r, axes(DOWN)[5], shard(DOWN, need[r], wrap(x + 1, 4), 1))

    def send_halves(r):
        half_up(r, 0)
        half_dn(r, 1)
        half_up(r, 1)
        half_dn(r, 0)

    def across_up(i, r):
        w_go(i, 4 + r, axes(i)[4], shard(i, order(i)[r], axes(i)[1]))

    def across_dn(i, r):
        w_go(i, 8 + r, axes(i)[5], shard(i, order(i)[r], axes(i)[1]))

    def got_up(i, r):
        w_got(i, 4 + r, shard(i, order(i)[r], wrap(axes(i)[1] - 1, 4)))

    def got_dn(i, r):
        w_got(i, 8 + r, shard(i, order(i)[r], wrap(axes(i)[1] + 1, 4)))

    def fwd_up(i, n):
        r, half = forwards(i)[0][n]
        if n == 0 or forwards(i)[0][n - 1][0] != r:
            got_up(i, r)
        w_go(i, 12 + n, axes(i)[4], shard(i, order(i)[r], wrap(axes(i)[1] - 1, 4), half))

    def fwd_dn(i, n):
        r, half = forwards(i)[1][n]
        got_dn(i, r)
        w_go(i, 15 + n, axes(i)[5], shard(i, order(i)[r], wrap(axes(i)[1] + 1, 4), half))

    def got_fwd_up(i, n):
        r, half = forwards(i)[0][n]
        w_got(i, 12 + n, shard(i, order(i)[r], wrap(axes(i)[1] + 2, 4), half))

    def got_fwd_dn(i, n):
        r, half = forwards(i)[1][n]
        w_got(i, 15 + n, shard(i, order(i)[r], wrap(axes(i)[1] + 2, 4), half))

    def share(i, k, region):
        w_go(i, k, other, region(core))

    def shared(i, k, region):
        w_got(i, k, region(1 - core))

    def row(i, n):
        sec = wrap(axes(i)[1] + (0, -1, 1)[n], 4)
        ref = items[i][0]
        return lambda cc: ref.at[cc, sec] if items[i][2] else ref.at[cc, :, sec]

    def single(i, r, step):
        f, sec = order(i)[r], wrap(axes(i)[1] + step, 4)
        return lambda cc: shard(i, f, sec, None, cc)

    def share_row(i, n):
        share(i, 18 + n, row(i, n))

    def share_far(i, r):
        share(i, 21 + r, single(i, r, 2))

    def all_shared(i):
        for n in range(3):
            shared(i, 18 + n, row(i, n))
        for r in (0, 2, 1, 3):
            shared(i, 21 + r, single(i, r, 2))

    def own_down(cc):
        return wd.at[cc, :, x]

    def share_down(r, n):
        share(DOWN, 19 + 3 * r + n, single(DOWN, r, (-1, 1, 2)[n]))

    def down_shared(r):
        for n in range(3):
            shared(DOWN, 19 + 3 * r + n, single(DOWN, r, (-1, 1, 2)[n]))

    for i in (GATE, UP, DOWN):
        w_copies[i].wait()
        step1(i)
    for i in (GATE, UP):
        across_up(i, 0)
        across_dn(i, 0)

    ones = jnp.ones((8, 128), F32)
    for c in small:
        c.wait()
    g32[...] = gain[...].astype(F32)

    def ps_copy(c, d, owner):
        return remote(
            pst.at[owner, :, pl.ds(c * CT, CT)], ps_send.at[c, d], ps_recv.at[c, d], z_peers[d]
        )

    for c in range(CHUNKS):
        st_copies[c].wait()
        tok = pl.ds(c * CT, CT)
        squares = jnp.zeros((CT, COLS), F32)
        raw = jnp.zeros((24, CT), F32)
        for k in range(STREAMS):
            v = st[k, tok, :]
            squares = squares + v * v
            raw = raw + nt_dot(mw[:, k, :], v)
        squares = (squares[:, :128] + squares[:, 128:256]) + (squares[:, 256:384] + squares[:, 384:])
        sq_row = nt_dot(ones, squares, lax.Precision.HIGHEST)
        pst[z, 0:4, tok] = raw[0:4]
        pst[z, 4:8, tok] = sq_row[4:8]
        ost[z, 0:20, tok] = raw[4:24]
        ost[z, 20:24, tok] = sq_row[4:8]
        for d in far_first:
            cp = ps_copy(c, d, z)
            cp.start()
            sends.append(cp)

    def hops(c, to_right):
        return 4 if (c % 2 == 0) == to_right else 3

    def ag_copy(c, h, to_right, origin):
        q = 0 if to_right else 1
        return remote(
            xg.at[origin, pl.ds(c * CT, CT), :], ag_send.at[q, c, h], ag_recv.at[q, c, h],
            right if to_right else left,
        )

    def ag_go(c, h, to_right, origin):
        cp = ag_copy(c, h, to_right, origin)
        cp.start()
        sends.append(cp)

    row8 = lax.broadcasted_iota(jnp.int32, (8, 1), 0)
    bias8 = jnp.zeros((8, 1), F32)
    for l in range(4):
        bias8 = jnp.where(row8 == l, bias[l], bias8)
    g_row = jnp.concatenate([g32[pl.ds(4 * z + q, 1), :] for q in range(4)], axis=1)

    def layer_input(c):
        tok = pl.ds(c * CT, CT)
        for d in far_first:
            ps_copy(c, d, wrap(z - d, NZ)).wait_recv()
        total = pst[0, :, tok]
        for o in range(1, NZ):
            total = total + pst[o, :, tok]
        inverse = lax.rsqrt(total[4:5] / float(STREAMS * COLS * NZ) + EPSILON)
        pre = jax.nn.sigmoid(scale[0] * (total * inverse) + bias8)
        pre = jnp.concatenate([pre, jnp.zeros((120, CT), F32)], axis=0)
        pre_t[tok, :] = pre.T
        layer_in = pre_t[tok, 0:1] * st[0, tok, :]
        for k in range(1, STREAMS):
            layer_in = layer_in + pre_t[tok, k : k + 1] * st[k, tok, :]
        sent = (layer_in * g_row).astype(BF16)
        for q in range(4):
            xg[z, tok, q * 128 : (q + 1) * 128] = sent[:, PERM[q] * 128 : (PERM[q] + 1) * 128]
        ag_go(c, 0, True, z)
        ag_go(c, 0, False, z)
        sq = layer_in * layer_in
        sq = (sq[:, :128] + sq[:, 128:256]) + (sq[:, 256:384] + sq[:, 384:])
        sqx[z, :, tok] = nt_dot(ones, sq, lax.Precision.HIGHEST)[0:1]

    for c in range(CHUNKS):
        layer_input(c)

    def ag_step(h, chunks):
        for c in chunks:
            for to_right in (True, False):
                if h < hops(c, to_right):
                    origin = wrap(z - (h + 1), NZ) if to_right else wrap(z + (h + 1), NZ)
                    ag_copy(c, h, to_right, origin).wait_recv()
                    if h + 1 < hops(c, to_right):
                        ag_go(c, h + 1, to_right, origin)

    for i in (GATE, UP):
        step2(i)
    for i in (UP, GATE):
        across_up(i, 1)
        across_dn(i, 2)
        across_up(i, 2)
        across_dn(i, 1)
    for d in far_first:
        cp = remote(sqx.at[z], sq_send.at[d], sq_recv.at[d], z_peers[d])
        cp.start()
        sends.append(cp)
    ag_step(0, (0, 1))
    step2(DOWN)
    ag_step(0, (2, 3))
    for i in (UP, GATE):
        step2_end(i)
        across_up(i, 3)
        across_dn(i, 3)
        share_row(i, 0)
    ag_step(1, (0, 1))
    fwd_up(UP, 0)
    fwd_up(UP, 1)
    fwd_dn(UP, 0)
    ag_step(1, (2, 3))
    fwd_dn(UP, 1)
    step2_end(DOWN)
    share(DOWN, 18, own_down)
    for up, dn in ((0, 1), (1, 0)):
        across_up(DOWN, up)
        across_dn(DOWN, dn)
    fwd_up(GATE, 0)
    fwd_up(GATE, 1)
    fwd_dn(GATE, 0)
    got_up(UP, 2)
    got_up(UP, 3)
    share_row(UP, 1)
    got_dn(UP, 0)
    got_dn(UP, 1)
    share_row(UP, 2)
    ag_step(2, (0, 1))
    got_fwd_up(UP, 0)
    share_far(UP, 0)
    got_fwd_dn(UP, 0)
    share_far(UP, 2)
    ag_step(2, (2,))
    fwd_dn(GATE, 1)
    got_up(GATE, 2)
    got_up(GATE, 3)
    share_row(GATE, 1)
    got_dn(GATE, 0)
    got_dn(GATE, 1)
    share_row(GATE, 2)
    ag_step(2, (3,))
    for d in far_first:
        cp = remote(ost.at[z], os_send.at[d], os_recv.at[d], z_peers[d])
        cp.start()
        sends.append(cp)
    got_fwd_up(UP, 1)
    share_far(UP, 1)
    got_fwd_dn(UP, 1)
    share_far(UP, 3)
    for d in far_first:
        remote(sqx.at[wrap(z - d, NZ)], sq_send.at[d], sq_recv.at[d], z_peers[d]).wait_recv()
    sq_total = sqx[0]
    for o in range(1, NZ):
        sq_total = sq_total + sqx[o]
    inv = lax.rsqrt(sq_total / float(COLS * NZ) + EPSILON)
    inv_t[...] = jnp.broadcast_to(inv, (128, TOK)).T
    ag_step(3, (0,))
    got_fwd_up(GATE, 0)
    share_far(GATE, 0)
    got_fwd_dn(GATE, 0)
    share_far(GATE, 2)
    fwd_up(DOWN, 0)
    fwd_dn(DOWN, 0)
    send_halves(2)
    share_down(0, 0)
    share_down(1, 1)
    ag_step(3, (1,))
    got_fwd_up(GATE, 1)
    share_far(GATE, 1)
    got_fwd_dn(GATE, 1)
    share_far(GATE, 3)
    all_shared(UP)
    all_shared(GATE)

    halves = 2
    ht = TOK // halves

    def gate_up(half, first, last):
        def tile(n, carry):
            tok = pl.ds(half * ht, ht)
            lanes = pl.ds(pl.multiple_of(n * 128, 128), 128)
            acc = None
            for b in range(NZ):
                for cc in range(2):
                    a = xg[b, tok, cc * 256 : (cc + 1) * 256]
                    j = 2 * (b % 2)
                    bg = wg[cc, b // 2, j : j + 2, :, lanes].reshape(256, 128)
                    bu = wu[cc, b // 2, j : j + 2, :, lanes].reshape(256, 128)
                    d = jnp.dot(a, jnp.concatenate([bg, bu], axis=1), preferred_element_type=F32)
                    acc = d if acc is None else acc + d
            scale_t = inv_t[tok, :]
            g = acc[:, :128] * scale_t
            u = acc[:, 128:] * scale_t
            hid[tok, lanes] = (g / (1.0 + jnp.exp(-g)) * u).astype(BF16)
            return carry

        lax.fori_loop(first, last, tile, 0, unroll=True)

    def partial(dest, tok):
        a = hid[tok, :]
        parts = []
        j = 2 * lax.rem(dest, 2)
        for cc in range(2):
            b0 = wd[cc, lax.div(dest, 2), j]
            b1 = wd[cc, lax.div(dest, 2), j + 1]
            parts.append(
                jnp.dot(a, jnp.concatenate([b0, b1], axis=1), preferred_element_type=F32)
            )
        return parts

    def rs_copy(q, c, t):
        src, dst = (sr, rr) if q == 0 else (sl, rl)
        return pltpu.make_async_remote_copy(
            src_ref=src.at[c, t], dst_ref=dst.at[c, t],
            send_sem=rs_send.at[q, c, t], recv_sem=rs_recv.at[q, c, t],
            device_id=right if q == 0 else left, device_id_type=MESH,
        )

    def first_lanes(own):
        return pl.ds(pl.multiple_of(256 * (core if own else 1 - core), 256), 256)

    def first_copy(q, c, own):
        src, dst = (sr, rr) if q == 0 else (sl, rl)
        lanes = first_lanes(own)
        k = 0 if own else 4
        return pltpu.make_async_remote_copy(
            src_ref=src.at[c, 0, :, lanes], dst_ref=dst.at[c, 0, :, lanes],
            send_sem=rs_send.at[q, c, k], recv_sem=rs_recv.at[q, c, k],
            device_id=right if q == 0 else left, device_id_type=MESH,
        )

    def rs_first(own, first, last):
        def chunk(c, carry):
            odd = lax.rem(c, 2)
            tok = pl.ds(pl.multiple_of(c * CT, CT), CT)
            for q in range(2):
                n_hops = 4 - odd if q == 0 else 3 + odd
                dest = wrap(z + n_hops, NZ) if q == 0 else wrap(z - n_hops, NZ)
                src = sr if q == 0 else sl
                j = 2 * lax.rem(dest, 2)
                cc = core if own else 1 - core
                b0 = wd[cc, lax.div(dest, 2), j]
                b1 = wd[cc, lax.div(dest, 2), j + 1]
                p = jnp.dot(
                    hid[tok, :], jnp.concatenate([b0, b1], axis=1), preferred_element_type=F32
                )
                src[c, 0, :, first_lanes(own)] = p.astype(BF16)
                first_copy(q, c, own).start()
            return carry

        lax.fori_loop(first, last, chunk, 0)

    def rs_step(t, first, last):
        def chunk(c, carry):
            odd = lax.rem(c, 2)
            tok = pl.ds(pl.multiple_of(c * CT, CT), CT)
            for q in range(2):
                n_hops = 4 - odd if q == 0 else 3 + odd

                def send():
                    dest = wrap(z + n_hops - t, NZ) if q == 0 else wrap(z - n_hops + t, NZ)
                    p0, p1 = partial(dest, tok)
                    src, dst = (sr, rr) if q == 0 else (sl, rl)
                    if t == 0:
                        src[c, t, :, 0:256] = p0.astype(BF16)
                        src[c, t, :, 256:512] = p1.astype(BF16)
                    else:
                        tmp[:, 0:256] = p0
                        tmp[:, 256:512] = p1
                        if t == 1 and first < 2:
                            first_copy(q, c, True).wait_recv()
                            first_copy(q, c, False).wait_recv()
                        else:
                            rs_copy(q, c, t - 1).wait_recv()
                        src[c, t] = (tmp[...] + dst[c, t - 1].astype(F32)).astype(BF16)
                    rs_copy(q, c, t).start()

                if t < 3:
                    send()
                else:
                    pl.when(n_hops == 4)(send)
            return carry

        lax.fori_loop(first, last, chunk, 0)

    gate_up(0, 0, 7)
    got_up(DOWN, 1)
    share_down(1, 0)
    got_dn(DOWN, 0)
    share_down(0, 1)
    ag_step(3, (2, 3))
    gate_up(1, 0, 1)
    got_fwd_up(DOWN, 0)
    share_down(0, 2)
    got_fwd_dn(DOWN, 0)
    share_down(1, 2)
    rs_first(True, 0, 2)
    gate_up(1, 1, 3)
    shared(DOWN, 18, own_down)
    down_shared(0)
    down_shared(1)
    rs_first(False, 0, 2)
    fwd_half_up(2)
    fwd_half_dn(2)
    send_halves(3)
    gate_up(1, 3, 7)
    rs_step(0, 2, 4)
    got_half_up(2, 1)
    share_down(2, 0)
    got_half_dn(2, 0)
    share_down(2, 1)
    got_fwd_up(DOWN, 1)
    got_fwd_dn(DOWN, 1)
    share_down(2, 2)
    down_shared(2)
    rs_step(1, 0, 2)
    fwd_half_up(3)
    fwd_half_dn(3)
    rs_step(1, 2, 4)
    got_half_up(3, 1)
    share_down(3, 0)
    got_half_dn(3, 0)
    share_down(3, 1)
    got_fwd_up(DOWN, 2)
    got_fwd_dn(DOWN, 2)
    share_down(3, 2)
    down_shared(3)

    for d in far_first:
        remote(ost.at[wrap(z - d, NZ)], os_send.at[d], os_recv.at[d], z_peers[d]).wait_recv()
    total = pst[0]
    rest = ost[0]
    for o in range(1, NZ):
        total = total + pst[o]
        rest = rest + ost[o]
    rest = rest * lax.rsqrt(total[4:5] / float(STREAMS * COLS * NZ) + EPSILON)
    row4 = lax.broadcasted_iota(jnp.int32, (4, 1), 0)

    def bias4(first):
        b = jnp.full((4, 1), bias[first], F32)
        for l in range(1, 4):
            b = jnp.where(row4 == l, bias[first + l], b)
        return b

    post = 2.0 * jax.nn.sigmoid(scale[1] * rest[0:4] + bias4(4))
    mix = tuple(
        jnp.exp(scale[2] * rest[4 + 4 * k : 8 + 4 * k] + bias4(8 + 4 * k)) for k in range(4)
    )

    def balance(_, m):
        m = tuple(v / jnp.sum(v, axis=0, keepdims=True) for v in m)
        col = (m[0] + m[1]) + (m[2] + m[3])
        return tuple(v / col for v in m)

    mix = lax.fori_loop(0, SWEEPS, balance, mix)
    coef = jnp.concatenate((post,) + mix + (jnp.zeros((108, TOK), F32),), axis=0)
    coef_t[...] = coef.T

    def post_write():
        return pltpu.make_async_copy(coef_t, post_hbm, out_sem.at[2 * CHUNKS])

    def base_write(c):
        tok = pl.ds(pl.multiple_of(c * CT, CT), CT)
        return pltpu.make_async_copy(base.at[:, tok, :], base_hbm.at[:, tok, :], out_sem.at[c])

    def lo_write(c):
        tok = pl.ds(pl.multiple_of(c * CT, CT), CT)
        return pltpu.make_async_copy(lo.at[tok, :], lo_hbm.at[tok, :], out_sem.at[CHUNKS + c])

    def residual(c):
        rows = 16

        def group(g, carry):
            tok = pl.ds(pl.multiple_of(c * CT + g * rows, rows), rows)
            wide = [
                jnp.broadcast_to(coef_t[tok, STREAMS + n : STREAMS + n + 1], (rows, 128))
                for n in range(STREAMS * STREAMS)
            ]
            for q in range(COLS // 128):
                lanes = slice(q * 128, (q + 1) * 128)
                src = [st[j, tok, lanes] for j in range(STREAMS)]
                for k in range(STREAMS):
                    v = wide[STREAMS * k] * src[0]
                    for j in range(1, STREAMS):
                        v = v + wide[STREAMS * k + j] * src[j]
                    base[k, tok, lanes] = v.astype(BF16)
            return carry

        lax.fori_loop(0, CT // rows, group, 0)
        base_write(c).start()

    post_write().start()
    residual(0)
    rs_step(2, 0, 2)
    residual(1)
    rs_step(2, 2, 4)
    for c in sends:
        c.wait_send()
    residual(2)
    rs_step(3, 0, 2)
    residual(3)
    rs_step(3, 2, 4)

    def own_body(c, carry):
        tok = pl.ds(pl.multiple_of(c * CT, CT), CT)
        p0, p1 = partial(z, tok)
        own[tok, 0:256] = p0
        own[tok, 256:512] = p1
        return carry

    lax.fori_loop(0, CHUNKS, own_body, 0)

    def out_body(c, carry):
        odd = lax.rem(c, 2)
        tok = pl.ds(pl.multiple_of(c * CT, CT), CT)
        rs_copy(0, c, 3 - odd).wait_recv()
        rs_copy(1, c, 2 + odd).wait_recv()
        for q in range(4):
            lanes = slice(q * 128, (q + 1) * 128)
            lo[tok, PERM[q] * 128 : (PERM[q] + 1) * 128] = (
                own[tok, lanes]
                + rr[c, 3 - odd, :, lanes].astype(F32)
                + rl[c, 2 + odd, :, lanes].astype(F32)
            )
        lo_write(c).start()
        return carry

    lax.fori_loop(0, CHUNKS, out_body, 0)

    for c in range(CHUNKS):
        for q in range(2):
            for t in range(hops(c, q == 0)):
                if t == 0 and c < 2:
                    first_copy(q, c, True).wait_send()
                    first_copy(q, c, False).wait_send()
                else:
                    rs_copy(q, c, t).wait_send()
    post_write().wait()
    for c in range(CHUNKS):
        base_write(c).wait()
        lo_write(c).wait()


def mix_kernel(base_hbm, lo_hbm, post_hbm, out_hbm, base, lo, post, out, in_sem, out_sem):
    def tokens(c):
        return pl.ds(c * MT, MT)

    def reads(c):
        return (
            pltpu.make_async_copy(post_hbm.at[tokens(c)], post.at[tokens(c)], in_sem.at[c, 0]),
            pltpu.make_async_copy(lo_hbm.at[tokens(c)], lo.at[tokens(c)], in_sem.at[c, 1]),
            pltpu.make_async_copy(base_hbm.at[:, tokens(c)], base.at[:, tokens(c)], in_sem.at[c, 2]),
        )

    def write(c):
        return pltpu.make_async_copy(out.at[:, tokens(c)], out_hbm.at[:, tokens(c)], out_sem.at[c])

    for c in range(TOK // MT):
        for copy in reads(c):
            copy.start()
    for c in range(TOK // MT):
        for copy in reads(c):
            copy.wait()
        tok = slice(c * MT, (c + 1) * MT)
        for k in range(STREAMS):
            out[k, tok, :] = base[k, tok, :].astype(F32) + post[tok, k : k + 1] * lo[tok, :]
        write(c).start()
    for c in range(TOK // MT):
        write(c).wait()


def body(streams, mix_weight, mix_bias, mix_scale, norm_gain, gate_weight, up_weight, down_weight):
    gain = norm_gain.reshape(NZ * 4, 128)
    hbm = pl.BlockSpec(memory_space=pltpu.HBM)
    dma = pltpu.SemaphoreType.DMA
    base, layer_out, post = pl.pallas_call(
        kernel,
        out_shape=(
            jax.ShapeDtypeStruct((STREAMS, TOK, COLS), BF16),
            jax.ShapeDtypeStruct((TOK, COLS), F32),
            jax.ShapeDtypeStruct((TOK, 128), F32),
        ),
        in_specs=[hbm] * 8,
        out_specs=(hbm, hbm, hbm),
        scratch_shapes=[
            pltpu.VMEM((STREAMS, TOK, COLS), F32),
            pltpu.VMEM((2, NY, NX, ROWS, FFL), BF16),
            pltpu.VMEM((2, NY, NX, ROWS, FFL), BF16),
            pltpu.VMEM((2, NY, NX, FFL, 128), BF16),
            pltpu.VMEM((NZ, TOK, COLS), BF16),
            pltpu.VMEM((TOK, FFL), BF16),
            pltpu.VMEM((CHUNKS, 4, CT, COLS), BF16),
            pltpu.VMEM((CHUNKS, 4, CT, COLS), BF16),
            pltpu.VMEM((CHUNKS, 4, CT, COLS), BF16),
            pltpu.VMEM((CHUNKS, 4, CT, COLS), BF16),
            pltpu.VMEM((NZ, 8, TOK), F32),
            pltpu.VMEM((NZ, 24, TOK), F32),
            pltpu.VMEM((NZ, 1, TOK), F32),
            pltpu.VMEM((TOK, 128), F32),
            pltpu.VMEM((TOK, 128), F32),
            pltpu.VMEM((CT, COLS), F32),
            pltpu.VMEM((NZ * 4, 128), F32),
            pltpu.VMEM((STREAMS, TOK, COLS), BF16),
            pltpu.VMEM((TOK, COLS), F32),
            pltpu.VMEM((TOK, COLS), F32),
            pltpu.VMEM((TOK, 128), F32),
            pltpu.VMEM((6 * STREAMS, STREAMS, COLS), F32),
            pltpu.SMEM((6 * STREAMS,), F32),
            pltpu.SMEM((3,), F32),
            pltpu.VMEM((NZ * 4, 128), BF16),
            dma((CHUNKS + 7,)),
            dma((2 * CHUNKS + 1,)),
            dma((3, 36)),
            dma((3, 36)),
            dma((2, CHUNKS, 4)),
            dma((2, CHUNKS, 4)),
            dma((2, CHUNKS, 5)),
            dma((2, CHUNKS, 5)),
            dma((CHUNKS, 8)),
            dma((CHUNKS, 8)),
            dma((8,)),
            dma((8,)),
            dma((8,)),
            dma((8,)),
        ],
        compiler_params=pltpu.CompilerParams(
            collective_id=0, has_side_effects=True, vmem_limit_bytes=60 * 1024 * 1024
        ),
    )(streams, mix_weight, mix_bias, mix_scale, gain, gate_weight, up_weight, down_weight)
    return pl.pallas_call(
        mix_kernel,
        out_shape=jax.ShapeDtypeStruct((STREAMS, TOK, COLS), F32),
        in_specs=[hbm, hbm, hbm],
        out_specs=hbm,
        scratch_shapes=[
            pltpu.VMEM((STREAMS, TOK, COLS), BF16),
            pltpu.VMEM((TOK, COLS), F32),
            pltpu.VMEM((TOK, 128), F32),
            pltpu.VMEM((STREAMS, TOK, COLS), F32),
            dma((TOK // MT, 3)),
            dma((TOK // MT,)),
        ],
        compiler_params=pltpu.CompilerParams(vmem_limit_bytes=60 * 1024 * 1024),
    )(base, layer_out, post)


def solution(mesh):
    placed = (
        P(None, "seq", "tensor"),
        P(None, None, "tensor"),
        P(),
        P(),
        P(),
        P("seq", "tensor"),
        P("seq", "tensor"),
        P("tensor", "seq"),
    )
    return jax.shard_map(
        body, mesh=mesh, in_specs=placed, out_specs=P(None, "seq", "tensor"), check_vma=False
    )
```

```python
import functools

import jax
import jax.numpy as jnp
from jax import lax
from jax.experimental import pallas as pl
from jax.experimental.pallas import tpu as pltpu
from jax.sharding import PartitionSpec as P

STREAMS = 4
SWEEPS = 20
EPSILON = 0.25
MESH = pl.DeviceIdType.MESH
NX = 4
NY = 4
NZ = 8
TOK = 512
COLS = 512
ROWS = 128
FFL = 896
CHUNKS = 4
CT = TOK // CHUNKS
MT = 64
PERM = (0, 2, 1, 3)
F32 = jnp.float32
BF16 = jnp.bfloat16


def wrap(value, size):
    return lax.rem(value + size, size)


def nt_dot(a, b, precision=None):
    return lax.dot_general(
        a, b, (((1,), (1,)), ((), ())), precision=precision, preferred_element_type=F32
    )


def kernel(
    st_hbm, mw_hbm, bias_hbm, scale_hbm, gain_hbm, g_hbm, u_hbm, d_hbm, base_hbm, lo_hbm, post_hbm,
    st, wg, wu, wd, xg, hid, rr, rl, sr, sl, pst, ost, sqx, pre_t, inv_t, tmp, g32,
    base, lo, own, coef_t, mw, bias, scale, gain, loc_sem, out_sem, w_send, w_recv, ag_send, ag_recv, rs_send, rs_recv,
    ps_send, ps_recv, os_send, os_recv, sq_send, sq_recv,
):
    s = lax.axis_index("seq")
    z = lax.axis_index("tensor")
    core = lax.rem(s, 2)
    x = lax.rem(lax.div(s, 2), NX)
    y = lax.div(s, 2 * NX)

    def at(xx, yy, cc):
        return {"seq": (yy * NX + xx) * 2 + cc, "tensor": z}

    x_up, x_dn = at(wrap(x + 1, NX), y, core), at(wrap(x - 1, NX), y, core)
    y_up, y_dn = at(x, wrap(y + 1, NY), core), at(x, wrap(y - 1, NY), core)
    other = at(x, y, 1 - core)
    right = {"seq": s, "tensor": wrap(z + 1, NZ)}
    left = {"seq": s, "tensor": wrap(z - 1, NZ)}
    z_peers = {d: {"seq": s, "tensor": wrap(z + d, NZ)} for d in range(1, NZ)}
    far_first = (4, 3, 5, 2, 6, 1, 7)

    w_copies = [
        pltpu.make_async_copy(src, dst.at[core, y, x], loc_sem.at[CHUNKS + i])
        for i, (src, dst) in enumerate(((g_hbm, wg), (u_hbm, wu), (d_hbm, wd)))
    ]
    st_copies = [
        pltpu.make_async_copy(
            st_hbm.at[:, pl.ds(c * CT, CT), :], st.at[:, pl.ds(c * CT, CT), :], loc_sem.at[c]
        )
        for c in range(CHUNKS)
    ]
    small = [
        pltpu.make_async_copy(src, dst, loc_sem.at[CHUNKS + 3 + i])
        for i, (src, dst) in enumerate(
            ((mw_hbm, mw), (gain_hbm, gain), (scale_hbm, scale), (bias_hbm, bias))
        )
    ]
    for c in w_copies + small + st_copies:
        c.start()

    barrier = pltpu.get_barrier_semaphore()
    peers = [x_up, x_dn, y_up, y_dn, other] + [z_peers[d] for d in range(1, NZ)]
    for peer in peers:
        pl.semaphore_signal(barrier, inc=1, device_id=peer, device_id_type=MESH)
    pl.semaphore_wait(barrier, len(peers))

    sends = []

    def remote(ref, send_sem, recv_sem, dev):
        return pltpu.make_async_remote_copy(
            src_ref=ref, dst_ref=ref, send_sem=send_sem, recv_sem=recv_sem,
            device_id=dev, device_id_type=MESH,
        )

    GATE, UP, DOWN = 0, 1, 2
    items = ((wg, ROWS, True), (wu, ROWS, False), (wd, FFL, False))

    def axes(i):
        if items[i][2]:
            return x, y, x_up, x_dn, y_up, y_dn
        return y, x, y_up, y_dn, x_up, x_dn

    def shard(i, f, sec, half=None, cc=None):
        ref, rows, x_first = items[i]
        cc = core if cc is None else cc
        rsl = slice(None) if half is None else pl.ds(half * (rows // 2), rows // 2)
        return ref.at[cc, sec, f, rsl, :] if x_first else ref.at[cc, f, sec, rsl, :]

    def w_copy(i, k, dev, region):
        return remote(region, w_send.at[i, k], w_recv.at[i, k], dev)

    def w_go(i, k, dev, region):
        c = w_copy(i, k, dev, region)
        c.start()
        sends.append(c)

    def w_got(i, k, region):
        w_copy(i, k, other, region).wait_recv()

    zq = lax.div(z, 2)
    zo = lax.rem(z, 2)
    need = [wrap(zq + 2, 4), wrap(zq + 1 + 2 * zo, 4), wrap(zq + 3 - 2 * zo, 4), wrap(zq, 4)]

    def order(i):
        f = axes(i)[0]
        if i == DOWN:
            return need
        return [f, wrap(f - 1, 4), wrap(f + 1, 4), wrap(f + 2, 4)]

    def forwards(i):
        if i == DOWN:
            return ((0, None), (2, 0), (3, 0)), ((1, None), (2, 1), (3, 1))
        return ((0, None), (1, None)), ((2, None), (3, None))

    def step1(i):
        f, sec, f_up, f_dn, _, _ = axes(i)
        w_go(i, 0, f_up, shard(i, f, sec))
        w_go(i, 1, f_dn, shard(i, f, sec))

    def step2(i):
        f, sec, f_up, f_dn, _, _ = axes(i)
        fm, fp = wrap(f - 1, 4), wrap(f + 1, 4)
        w_got(i, 0, shard(i, fm, sec))
        w_go(i, 2, f_up, shard(i, fm, sec, 0))
        w_got(i, 1, shard(i, fp, sec))
        w_go(i, 3, f_dn, shard(i, fp, sec, 1))

    def step2_end(i):
        f, sec = axes(i)[:2]
        w_got(i, 2, shard(i, wrap(f + 2, 4), sec, 0))
        w_got(i, 3, shard(i, wrap(f + 2, 4), sec, 1))

    def half_up(r, n):
        k = 4 + r if n == 0 else 30 + r
        w_go(DOWN, k, axes(DOWN)[4], shard(DOWN, need[r], x, n))

    def half_dn(r, n):
        k = 8 + r if n == 1 else 32 + r
        w_go(DOWN, k, axes(DOWN)[5], shard(DOWN, need[r], x, n))

    def got_half_up(r, n):
        w_got(DOWN, 4 + r if n == 0 else 30 + r, shard(DOWN, need[r], wrap(x - 1, 4), n))

    def got_half_dn(r, n):
        w_got(DOWN, 8 + r if n == 1 else 32 + r, shard(DOWN, need[r], wrap(x + 1, 4), n))

    def fwd_half_up(r):
        got_half_up(r, 0)
        w_go(DOWN, 11 + r, axes(DOWN)[4], shard(DOWN, need[r], wrap(x - 1, 4), 0))

    def fwd_half_dn(r):
        got_half_dn(r, 1)
        w_go(DOWN, 14 + r, axes(DOWN)[5], shard(DOWN, need[r], wrap(x + 1, 4), 1))

    def send_halves(r):
        half_up(r, 0)
        half_dn(r, 1)
        half_up(r, 1)
        half_dn(r, 0)

    def across_up(i, r):
        w_go(i, 4 + r, axes(i)[4], shard(i, order(i)[r], axes(i)[1]))

    def across_dn(i, r):
        w_go(i, 8 + r, axes(i)[5], shard(i, order(i)[r], axes(i)[1]))

    def got_up(i, r):
        w_got(i, 4 + r, shard(i, order(i)[r], wrap(axes(i)[1] - 1, 4)))

    def got_dn(i, r):
        w_got(i, 8 + r, shard(i, order(i)[r], wrap(axes(i)[1] + 1, 4)))

    def fwd_up(i, n):
        r, half = forwards(i)[0][n]
        if n == 0 or forwards(i)[0][n - 1][0] != r:
            got_up(i, r)
        w_go(i, 12 + n, axes(i)[4], shard(i, order(i)[r], wrap(axes(i)[1] - 1, 4), half))

    def fwd_dn(i, n):
        r, half = forwards(i)[1][n]
        got_dn(i, r)
        w_go(i, 15 + n, axes(i)[5], shard(i, order(i)[r], wrap(axes(i)[1] + 1, 4), half))

    def got_fwd_up(i, n):
        r, half = forwards(i)[0][n]
        w_got(i, 12 + n, shard(i, order(i)[r], wrap(axes(i)[1] + 2, 4), half))

    def got_fwd_dn(i, n):
        r, half = forwards(i)[1][n]
        w_got(i, 15 + n, shard(i, order(i)[r], wrap(axes(i)[1] + 2, 4), half))

    def share(i, k, region):
        w_go(i, k, other, region(core))

    def shared(i, k, region):
        w_got(i, k, region(1 - core))

    def row(i, n):
        sec = wrap(axes(i)[1] + (0, -1, 1)[n], 4)
        ref = items[i][0]
        return lambda cc: ref.at[cc, sec] if items[i][2] else ref.at[cc, :, sec]

    def single(i, r, step):
        f, sec = order(i)[r], wrap(axes(i)[1] + step, 4)
        return lambda cc: shard(i, f, sec, None, cc)

    def share_row(i, n):
        share(i, 18 + n, row(i, n))

    def share_far(i, r):
        share(i, 21 + r, single(i, r, 2))

    def all_shared(i):
        for n in range(3):
            shared(i, 18 + n, row(i, n))
        for r in (0, 2, 1, 3):
            shared(i, 21 + r, single(i, r, 2))

    def own_down(cc):
        return wd.at[cc, :, x]

    def share_down(r, n):
        share(DOWN, 19 + 3 * r + n, single(DOWN, r, (-1, 1, 2)[n]))

    def down_shared(r):
        for n in range(3):
            shared(DOWN, 19 + 3 * r + n, single(DOWN, r, (-1, 1, 2)[n]))

    for i in (GATE, UP, DOWN):
        w_copies[i].wait()
        step1(i)
    for i in (GATE, UP):
        across_up(i, 0)
        across_dn(i, 0)

    ones = jnp.ones((8, 128), F32)
    for c in small:
        c.wait()
    g32[...] = gain[...].astype(F32)

    def ps_copy(c, d, owner):
        return remote(
            pst.at[owner, :, pl.ds(c * CT, CT)], ps_send.at[c, d], ps_recv.at[c, d], z_peers[d]
        )

    for c in range(CHUNKS):
        st_copies[c].wait()
        tok = pl.ds(c * CT, CT)
        squares = jnp.zeros((CT, COLS), F32)
        raw = jnp.zeros((24, CT), F32)
        for k in range(STREAMS):
            v = st[k, tok, :]
            squares = squares + v * v
            raw = raw + nt_dot(mw[:, k, :], v)
        squares = (squares[:, :128] + squares[:, 128:256]) + (squares[:, 256:384] + squares[:, 384:])
        sq_row = nt_dot(ones, squares, lax.Precision.HIGHEST)
        pst[z, 0:4, tok] = raw[0:4]
        pst[z, 4:8, tok] = sq_row[4:8]
        ost[z, 0:20, tok] = raw[4:24]
        ost[z, 20:24, tok] = sq_row[4:8]
        for d in far_first:
            cp = ps_copy(c, d, z)
            cp.start()
            sends.append(cp)

    def hops(c, to_right):
        return 4 if (c % 2 == 0) == to_right else 3

    def ag_copy(c, h, to_right, origin):
        q = 0 if to_right else 1
        return remote(
            xg.at[origin, pl.ds(c * CT, CT), :], ag_send.at[q, c, h], ag_recv.at[q, c, h],
            right if to_right else left,
        )

    def ag_go(c, h, to_right, origin):
        cp = ag_copy(c, h, to_right, origin)
        cp.start()
        sends.append(cp)

    row8 = lax.broadcasted_iota(jnp.int32, (8, 1), 0)
    bias8 = jnp.zeros((8, 1), F32)
    for l in range(4):
        bias8 = jnp.where(row8 == l, bias[l], bias8)
    g_row = jnp.concatenate([g32[pl.ds(4 * z + q, 1), :] for q in range(4)], axis=1)

    def layer_input(c):
        tok = pl.ds(c * CT, CT)
        for d in far_first:
            ps_copy(c, d, wrap(z - d, NZ)).wait_recv()
        total = pst[0, :, tok]
        for o in range(1, NZ):
            total = total + pst[o, :, tok]
        inverse = lax.rsqrt(total[4:5] / float(STREAMS * COLS * NZ) + EPSILON)
        pre = jax.nn.sigmoid(scale[0] * (total * inverse) + bias8)
        pre = jnp.concatenate([pre, jnp.zeros((120, CT), F32)], axis=0)
        pre_t[tok, :] = pre.T
        layer_in = pre_t[tok, 0:1] * st[0, tok, :]
        for k in range(1, STREAMS):
            layer_in = layer_in + pre_t[tok, k : k + 1] * st[k, tok, :]
        sent = (layer_in * g_row).astype(BF16)
        for q in range(4):
            xg[z, tok, q * 128 : (q + 1) * 128] = sent[:, PERM[q] * 128 : (PERM[q] + 1) * 128]
        ag_go(c, 0, True, z)
        ag_go(c, 0, False, z)
        sq = layer_in * layer_in
        sq = (sq[:, :128] + sq[:, 128:256]) + (sq[:, 256:384] + sq[:, 384:])
        sqx[z, :, tok] = nt_dot(ones, sq, lax.Precision.HIGHEST)[0:1]

    for c in range(CHUNKS):
        layer_input(c)

    def ag_step(h, chunks):
        for c in chunks:
            for to_right in (True, False):
                if h < hops(c, to_right):
                    origin = wrap(z - (h + 1), NZ) if to_right else wrap(z + (h + 1), NZ)
                    ag_copy(c, h, to_right, origin).wait_recv()
                    if h + 1 < hops(c, to_right):
                        ag_go(c, h + 1, to_right, origin)

    for i in (GATE, UP):
        step2(i)
    for i in (UP, GATE):
        across_up(i, 1)
        across_dn(i, 2)
        across_up(i, 2)
        across_dn(i, 1)
    for d in far_first:
        cp = remote(sqx.at[z], sq_send.at[d], sq_recv.at[d], z_peers[d])
        cp.start()
        sends.append(cp)
    ag_step(0, (0, 1))
    step2(DOWN)
    ag_step(0, (2, 3))
    for i in (UP, GATE):
        step2_end(i)
        across_up(i, 3)
        across_dn(i, 3)
        share_row(i, 0)
    ag_step(1, (0, 1))
    fwd_up(UP, 0)
    fwd_up(UP, 1)
    fwd_dn(UP, 0)
    ag_step(1, (2, 3))
    fwd_dn(UP, 1)
    step2_end(DOWN)
    share(DOWN, 18, own_down)
    for up, dn in ((0, 1), (1, 0)):
        across_up(DOWN, up)
        across_dn(DOWN, dn)
    fwd_up(GATE, 0)
    fwd_up(GATE, 1)
    fwd_dn(GATE, 0)
    got_up(UP, 2)
    got_up(UP, 3)
    share_row(UP, 1)
    got_dn(UP, 0)
    got_dn(UP, 1)
    share_row(UP, 2)
    ag_step(2, (0, 1))
    got_fwd_up(UP, 0)
    share_far(UP, 0)
    got_fwd_dn(UP, 0)
    share_far(UP, 2)
    ag_step(2, (2,))
    fwd_dn(GATE, 1)
    got_up(GATE, 2)
    got_up(GATE, 3)
    share_row(GATE, 1)
    got_dn(GATE, 0)
    got_dn(GATE, 1)
    share_row(GATE, 2)
    ag_step(2, (3,))
    for d in far_first:
        cp = remote(ost.at[z], os_send.at[d], os_recv.at[d], z_peers[d])
        cp.start()
        sends.append(cp)
    got_fwd_up(UP, 1)
    share_far(UP, 1)
    got_fwd_dn(UP, 1)
    share_far(UP, 3)
    for d in far_first:
        remote(sqx.at[wrap(z - d, NZ)], sq_send.at[d], sq_recv.at[d], z_peers[d]).wait_recv()
    sq_total = sqx[0]
    for o in range(1, NZ):
        sq_total = sq_total + sqx[o]
    inv = lax.rsqrt(sq_total / float(COLS * NZ) + EPSILON)
    inv_t[...] = jnp.broadcast_to(inv, (128, TOK)).T
    ag_step(3, (0,))
    got_fwd_up(GATE, 0)
    share_far(GATE, 0)
    got_fwd_dn(GATE, 0)
    share_far(GATE, 2)
    fwd_up(DOWN, 0)
    fwd_dn(DOWN, 0)
    send_halves(2)
    share_down(0, 0)
    share_down(1, 1)
    ag_step(3, (1,))
    got_fwd_up(GATE, 1)
    share_far(GATE, 1)
    got_fwd_dn(GATE, 1)
    share_far(GATE, 3)
    all_shared(UP)
    all_shared(GATE)

    halves = 2
    ht = TOK // halves

    def gate_up(half, first, last):
        def tile(n, carry):
            tok = pl.ds(half * ht, ht)
            lanes = pl.ds(pl.multiple_of(n * 128, 128), 128)
            acc = None
            for b in range(NZ):
                for cc in range(2):
                    a = xg[b, tok, cc * 256 : (cc + 1) * 256]
                    j = 2 * (b % 2)
                    bg = wg[cc, b // 2, j : j + 2, :, lanes].reshape(256, 128)
                    bu = wu[cc, b // 2, j : j + 2, :, lanes].reshape(256, 128)
                    d = jnp.dot(a, jnp.concatenate([bg, bu], axis=1), preferred_element_type=F32)
                    acc = d if acc is None else acc + d
            scale_t = inv_t[tok, :]
            g = acc[:, :128] * scale_t
            u = acc[:, 128:] * scale_t
            hid[tok, lanes] = (g / (1.0 + jnp.exp(-g)) * u).astype(BF16)
            return carry

        lax.fori_loop(first, last, tile, 0, unroll=True)

    def partial(dest, tok):
        a = hid[tok, :]
        parts = []
        j = 2 * lax.rem(dest, 2)
        for cc in range(2):
            b0 = wd[cc, lax.div(dest, 2), j]
            b1 = wd[cc, lax.div(dest, 2), j + 1]
            parts.append(
                jnp.dot(a, jnp.concatenate([b0, b1], axis=1), preferred_element_type=F32)
            )
        return parts

    def rs_copy(q, c, t):
        src, dst = (sr, rr) if q == 0 else (sl, rl)
        return pltpu.make_async_remote_copy(
            src_ref=src.at[c, t], dst_ref=dst.at[c, t],
            send_sem=rs_send.at[q, c, t], recv_sem=rs_recv.at[q, c, t],
            device_id=right if q == 0 else left, device_id_type=MESH,
        )

    def first_lanes(own):
        return pl.ds(pl.multiple_of(256 * (core if own else 1 - core), 256), 256)

    def first_copy(q, c, own):
        src, dst = (sr, rr) if q == 0 else (sl, rl)
        lanes = first_lanes(own)
        k = 0 if own else 4
        return pltpu.make_async_remote_copy(
            src_ref=src.at[c, 0, :, lanes], dst_ref=dst.at[c, 0, :, lanes],
            send_sem=rs_send.at[q, c, k], recv_sem=rs_recv.at[q, c, k],
            device_id=right if q == 0 else left, device_id_type=MESH,
        )

    def rs_first(own):
        cc = core if own else 1 - core
        lanes = first_lanes(own)

        def product(dest, tok):
            j = 2 * lax.rem(dest, 2)
            b0 = wd[cc, lax.div(dest, 2), j]
            b1 = wd[cc, lax.div(dest, 2), j + 1]
            both = jnp.concatenate([b0, b1], axis=1)
            return jnp.dot(hid[tok, :], both, preferred_element_type=F32).astype(BF16)

        far = product(wrap(z + 4, NZ), slice(0, 2 * CT))
        sr[0, 0, :, lanes] = far[:CT]
        sl[1, 0, :, lanes] = far[CT:]
        first_copy(0, 0, own).start()
        first_copy(1, 1, own).start()
        sl[0, 0, :, lanes] = product(wrap(z - 3, NZ), slice(0, CT))
        first_copy(1, 0, own).start()
        sr[1, 0, :, lanes] = product(wrap(z + 3, NZ), slice(CT, 2 * CT))
        first_copy(0, 1, own).start()

    def rs_step(t, first, last):
        def chunk(c, carry):
            odd = lax.rem(c, 2)
            tok = pl.ds(pl.multiple_of(c * CT, CT), CT)
            for q in range(2):
                n_hops = 4 - odd if q == 0 else 3 + odd

                def send():
                    dest = wrap(z + n_hops - t, NZ) if q == 0 else wrap(z - n_hops + t, NZ)
                    p0, p1 = partial(dest, tok)
                    src, dst = (sr, rr) if q == 0 else (sl, rl)
                    if t == 0:
                        src[c, t, :, 0:256] = p0.astype(BF16)
                        src[c, t, :, 256:512] = p1.astype(BF16)
                    else:
                        tmp[:, 0:256] = p0
                        tmp[:, 256:512] = p1
                        if t == 1 and first < 2:
                            first_copy(q, c, True).wait_recv()
                            first_copy(q, c, False).wait_recv()
                        else:
                            rs_copy(q, c, t - 1).wait_recv()
                        src[c, t] = (tmp[...] + dst[c, t - 1].astype(F32)).astype(BF16)
                    rs_copy(q, c, t).start()

                if t < 3:
                    send()
                else:
                    pl.when(n_hops == 4)(send)
            return carry

        lax.fori_loop(first, last, chunk, 0)

    gate_up(0, 0, 7)
    got_up(DOWN, 1)
    share_down(1, 0)
    got_dn(DOWN, 0)
    share_down(0, 1)
    ag_step(3, (2, 3))
    gate_up(1, 0, 1)
    got_fwd_up(DOWN, 0)
    share_down(0, 2)
    got_fwd_dn(DOWN, 0)
    share_down(1, 2)
    rs_first(True)
    gate_up(1, 1, 3)
    shared(DOWN, 18, own_down)
    down_shared(0)
    down_shared(1)
    rs_first(False)
    fwd_half_up(2)
    fwd_half_dn(2)
    send_halves(3)
    gate_up(1, 3, 7)
    rs_step(0, 2, 4)
    got_half_up(2, 1)
    share_down(2, 0)
    got_half_dn(2, 0)
    share_down(2, 1)
    got_fwd_up(DOWN, 1)
    got_fwd_dn(DOWN, 1)
    share_down(2, 2)
    down_shared(2)
    rs_step(1, 0, 2)
    fwd_half_up(3)
    fwd_half_dn(3)
    rs_step(1, 2, 4)
    got_half_up(3, 1)
    share_down(3, 0)
    got_half_dn(3, 0)
    share_down(3, 1)
    got_fwd_up(DOWN, 2)
    got_fwd_dn(DOWN, 2)
    share_down(3, 2)
    down_shared(3)

    for d in far_first:
        remote(ost.at[wrap(z - d, NZ)], os_send.at[d], os_recv.at[d], z_peers[d]).wait_recv()
    total = pst[0]
    rest = ost[0]
    for o in range(1, NZ):
        total = total + pst[o]
        rest = rest + ost[o]
    rest = rest * lax.rsqrt(total[4:5] / float(STREAMS * COLS * NZ) + EPSILON)
    row4 = lax.broadcasted_iota(jnp.int32, (4, 1), 0)

    def bias4(first):
        b = jnp.full((4, 1), bias[first], F32)
        for l in range(1, 4):
            b = jnp.where(row4 == l, bias[first + l], b)
        return b

    post = 2.0 * jax.nn.sigmoid(scale[1] * rest[0:4] + bias4(4))
    mix = tuple(
        jnp.exp(scale[2] * rest[4 + 4 * k : 8 + 4 * k] + bias4(8 + 4 * k)) for k in range(4)
    )

    def balance(_, m):
        m = tuple(v / jnp.sum(v, axis=0, keepdims=True) for v in m)
        col = (m[0] + m[1]) + (m[2] + m[3])
        return tuple(v / col for v in m)

    mix = lax.fori_loop(0, SWEEPS, balance, mix)
    coef = jnp.concatenate((post,) + mix + (jnp.zeros((108, TOK), F32),), axis=0)
    coef_t[...] = coef.T

    def post_write():
        return pltpu.make_async_copy(coef_t, post_hbm, out_sem.at[2 * CHUNKS])

    def base_write(c):
        tok = pl.ds(pl.multiple_of(c * CT, CT), CT)
        return pltpu.make_async_copy(base.at[:, tok, :], base_hbm.at[:, tok, :], out_sem.at[c])

    def lo_write(c):
        tok = pl.ds(pl.multiple_of(c * CT, CT), CT)
        return pltpu.make_async_copy(lo.at[tok, :], lo_hbm.at[tok, :], out_sem.at[CHUNKS + c])

    def residual(c):
        rows = 16

        def group(g, carry):
            tok = pl.ds(pl.multiple_of(c * CT + g * rows, rows), rows)
            wide = [
                jnp.broadcast_to(coef_t[tok, STREAMS + n : STREAMS + n + 1], (rows, 128))
                for n in range(STREAMS * STREAMS)
            ]
            for q in range(COLS // 128):
                lanes = slice(q * 128, (q + 1) * 128)
                src = [st[j, tok, lanes] for j in range(STREAMS)]
                for k in range(STREAMS):
                    v = wide[STREAMS * k] * src[0]
                    for j in range(1, STREAMS):
                        v = v + wide[STREAMS * k + j] * src[j]
                    base[k, tok, lanes] = v.astype(BF16)
            return carry

        lax.fori_loop(0, CT // rows, group, 0)
        base_write(c).start()

    post_write().start()
    residual(0)
    rs_step(2, 0, 2)
    residual(1)
    rs_step(2, 2, 4)
    for c in sends:
        c.wait_send()
    residual(2)
    rs_step(3, 0, 2)
    residual(3)
    rs_step(3, 2, 4)

    def own_body(c, carry):
        tok = pl.ds(pl.multiple_of(c * CT, CT), CT)
        p0, p1 = partial(z, tok)
        own[tok, 0:256] = p0
        own[tok, 256:512] = p1
        return carry

    lax.fori_loop(0, CHUNKS, own_body, 0)

    def out_body(c, carry):
        odd = lax.rem(c, 2)
        tok = pl.ds(pl.multiple_of(c * CT, CT), CT)
        rs_copy(0, c, 3 - odd).wait_recv()
        rs_copy(1, c, 2 + odd).wait_recv()
        for q in range(4):
            lanes = slice(q * 128, (q + 1) * 128)
            lo[tok, PERM[q] * 128 : (PERM[q] + 1) * 128] = (
                own[tok, lanes]
                + rr[c, 3 - odd, :, lanes].astype(F32)
                + rl[c, 2 + odd, :, lanes].astype(F32)
            )
        lo_write(c).start()
        return carry

    lax.fori_loop(0, CHUNKS, out_body, 0)

    for c in range(CHUNKS):
        for q in range(2):
            for t in range(hops(c, q == 0)):
                if t == 0 and c < 2:
                    first_copy(q, c, True).wait_send()
                    first_copy(q, c, False).wait_send()
                else:
                    rs_copy(q, c, t).wait_send()
    post_write().wait()
    for c in range(CHUNKS):
        base_write(c).wait()
        lo_write(c).wait()


def mix_kernel(base_hbm, lo_hbm, post_hbm, out_hbm, base, lo, post, out, in_sem, out_sem):
    def tokens(c):
        return pl.ds(c * MT, MT)

    def reads(c):
        return (
            pltpu.make_async_copy(post_hbm.at[tokens(c)], post.at[tokens(c)], in_sem.at[c, 0]),
            pltpu.make_async_copy(lo_hbm.at[tokens(c)], lo.at[tokens(c)], in_sem.at[c, 1]),
            pltpu.make_async_copy(base_hbm.at[:, tokens(c)], base.at[:, tokens(c)], in_sem.at[c, 2]),
        )

    def write(c):
        return pltpu.make_async_copy(out.at[:, tokens(c)], out_hbm.at[:, tokens(c)], out_sem.at[c])

    for c in range(TOK // MT):
        for copy in reads(c):
            copy.start()
    for c in range(TOK // MT):
        for copy in reads(c):
            copy.wait()
        tok = slice(c * MT, (c + 1) * MT)
        for k in range(STREAMS):
            out[k, tok, :] = base[k, tok, :].astype(F32) + post[tok, k : k + 1] * lo[tok, :]
        write(c).start()
    for c in range(TOK // MT):
        write(c).wait()


def body(streams, mix_weight, mix_bias, mix_scale, norm_gain, gate_weight, up_weight, down_weight):
    gain = norm_gain.reshape(NZ * 4, 128)
    hbm = pl.BlockSpec(memory_space=pltpu.HBM)
    dma = pltpu.SemaphoreType.DMA
    base, layer_out, post = pl.pallas_call(
        kernel,
        out_shape=(
            jax.ShapeDtypeStruct((STREAMS, TOK, COLS), BF16),
            jax.ShapeDtypeStruct((TOK, COLS), F32),
            jax.ShapeDtypeStruct((TOK, 128), F32),
        ),
        in_specs=[hbm] * 8,
        out_specs=(hbm, hbm, hbm),
        scratch_shapes=[
            pltpu.VMEM((STREAMS, TOK, COLS), F32),
            pltpu.VMEM((2, NY, NX, ROWS, FFL), BF16),
            pltpu.VMEM((2, NY, NX, ROWS, FFL), BF16),
            pltpu.VMEM((2, NY, NX, FFL, 128), BF16),
            pltpu.VMEM((NZ, TOK, COLS), BF16),
            pltpu.VMEM((TOK, FFL), BF16),
            pltpu.VMEM((CHUNKS, 4, CT, COLS), BF16),
            pltpu.VMEM((CHUNKS, 4, CT, COLS), BF16),
            pltpu.VMEM((CHUNKS, 4, CT, COLS), BF16),
            pltpu.VMEM((CHUNKS, 4, CT, COLS), BF16),
            pltpu.VMEM((NZ, 8, TOK), F32),
            pltpu.VMEM((NZ, 24, TOK), F32),
            pltpu.VMEM((NZ, 1, TOK), F32),
            pltpu.VMEM((TOK, 128), F32),
            pltpu.VMEM((TOK, 128), F32),
            pltpu.VMEM((CT, COLS), F32),
            pltpu.VMEM((NZ * 4, 128), F32),
            pltpu.VMEM((STREAMS, TOK, COLS), BF16),
            pltpu.VMEM((TOK, COLS), F32),
            pltpu.VMEM((TOK, COLS), F32),
            pltpu.VMEM((TOK, 128), F32),
            pltpu.VMEM((6 * STREAMS, STREAMS, COLS), F32),
            pltpu.SMEM((6 * STREAMS,), F32),
            pltpu.SMEM((3,), F32),
            pltpu.VMEM((NZ * 4, 128), BF16),
            dma((CHUNKS + 7,)),
            dma((2 * CHUNKS + 1,)),
            dma((3, 36)),
            dma((3, 36)),
            dma((2, CHUNKS, 4)),
            dma((2, CHUNKS, 4)),
            dma((2, CHUNKS, 5)),
            dma((2, CHUNKS, 5)),
            dma((CHUNKS, 8)),
            dma((CHUNKS, 8)),
            dma((8,)),
            dma((8,)),
            dma((8,)),
            dma((8,)),
        ],
        compiler_params=pltpu.CompilerParams(
            collective_id=0, has_side_effects=True, vmem_limit_bytes=60 * 1024 * 1024
        ),
    )(streams, mix_weight, mix_bias, mix_scale, gain, gate_weight, up_weight, down_weight)
    return pl.pallas_call(
        mix_kernel,
        out_shape=jax.ShapeDtypeStruct((STREAMS, TOK, COLS), F32),
        in_specs=[hbm, hbm, hbm],
        out_specs=hbm,
        scratch_shapes=[
            pltpu.VMEM((STREAMS, TOK, COLS), BF16),
            pltpu.VMEM((TOK, COLS), F32),
            pltpu.VMEM((TOK, 128), F32),
            pltpu.VMEM((STREAMS, TOK, COLS), F32),
            dma((TOK // MT, 3)),
            dma((TOK // MT,)),
        ],
        compiler_params=pltpu.CompilerParams(vmem_limit_bytes=60 * 1024 * 1024),
    )(base, layer_out, post)


def solution(mesh):
    placed = (
        P(None, "seq", "tensor"),
        P(None, None, "tensor"),
        P(),
        P(),
        P(),
        P("seq", "tensor"),
        P("seq", "tensor"),
        P("tensor", "seq"),
    )
    return jax.shard_map(
        body, mesh=mesh, in_specs=placed, out_specs=P(None, "seq", "tensor"), check_vma=False
    )
```
